256 devices in a mesh: mem: 16 (over z, core), dom: 16 (over x, y).
Axes of the slice: x: 4, y: 4, z: 8, core: 2. Of those that a mesh axis runs over, the one named last changes fastest.
Arguments:
- prior_ensemble: float32 [64, 4, 2048, 512], P('mem', None, 'dom'), may hold values from -6 to 6
- spreading_factor: float32 [4], replicated, may hold values from 0.05 to 0.24
- tendency_matrix: float32 [4, 4], replicated, may hold values from -0.6 to 0.6
- measured_data: float32 [16, 8192], P('dom', 'mem'), may hold values from -6 to 6
- inverse_error: float32 [16, 8192], P('dom', 'mem'), may hold values from 0.1 to 1
- assigned_subregion: int32 [16, 8192, 1], P('dom', 'mem'), may hold values from 0 to 31; in each aligned block of 512 rows (0 to 511, 512 to 1023, ..., all dimensions but the last counted through in order) at most 32 rows name the same one
- measured_entry: int32 [16, 8192], P('dom', 'mem'), may hold values from 0 to 8191
- taper_index: int32 [16, 8192], P('dom', 'mem'), may hold values from 0 to 63
- taper_factors: float32 [64], replicated, may hold values from 0.2 to 1
Outputs:
- analysis: float32 [64, 4, 2048, 512], P('mem', None, 'dom')
The draws below stay inside these ranges and needn't reach their ends.
Inputs may be any that keep to these rules, and one draw needn't show every extreme that they name: `assigned_subregion`: in the rows of one device no patch is named by more than 32 rows, a bound that some block reaches.
All inputs are finite; a program needn't handle non-finite values.
Results may differ from the reference program's by a relative error of at most 0.0003.
Values sent between devices are 32-bit elements; how exact they have to be, the bound alone decides.
No kernel may reach another device: no remote copies, remote signals or barrier semaphores. Data moves between devices by JAX's collectives and lax.ppermute only.
A program may use at most 64 MiB of HBM per device.

```python
import math
import jax
import jax.numpy as jnp
import numpy as np
from jax import lax

ENSEMBLE_SIZE = 64
PROGNOSTIC_VARS = 4
PATCH = 2048
SUBDOMAIN_LINES = 128
EAST_WEST_SPAN = 512
OBS_DEV = 512
NS_ITERS = 5
LOC_LEVELS = 64
NORTH_SOUTH_SPAN = 2048
PATCH_TILE = 32
OBS_CAP = 32
OBS_TILE = 8192
N_DOM = 16


def plant(entries, own_key, smallest, high):
    shape = entries.shape
    place = [jax.random.randint(jax.random.fold_in(own_key, axis), (), 0, shape[axis]) for axis in range(len(shape))]
    entries = entries.at[tuple(place)].set(smallest)
    longest = shape.index(max(shape))
    place[longest] = (place[longest] + 1) % shape[longest]
    return entries.at[tuple(place)].set(high)


def block_levels(rng, extent, cuts, least, top_value):
    def one(dim, blocks):
        draws = jax.random.uniform(jax.random.fold_in(jax.random.fold_in(rng, 6), dim), (blocks,), jnp.float32, least / len(cuts), top_value / len(cuts))
        return jnp.repeat(jnp.exp(draws), extent[dim] // blocks).reshape((-1,) + (1,) * (len(extent) - dim - 1))

    gain = one(*cuts[0])
    for cut in cuts[1:]:
        gain = gain * one(*cut)
    return gain


def deal_out(key, own, number, rows, number_of, top, bound, slope):
    sequence = jax.random.permutation(key, number_of)
    packed, common = portions_of(number_of, rows * top, bound, slope, True), portions_of(number_of, rows * top, bound, slope, False)
    places = jnp.arange(number_of)

    def named(tallies, offset_by):
        used = int((tallies > 0).sum())
        fixed = max(1, used // 4)
        passed = fixed + (places - fixed + offset_by * (used - fixed)) % max(1, number_of - fixed)
        return jnp.zeros((number_of,), jnp.int32).at[sequence[jnp.where(places < fixed, places, passed)]].set(jnp.asarray(tallies, jnp.int32))

    tallies = jnp.where(number % 4 == 0, named(packed, number // 4), named(common, number - number // 4 - 1))
    mixed = jax.random.permutation(jax.random.fold_in(own, 3), number_of)
    giver, sink = mixed[0:number_of // 2 * 2:2], mixed[1:number_of // 2 * 2:2]
    margin = jnp.minimum(tallies[giver] - 1, bound - tallies[sink]) // 2
    margin = jnp.where((giver == sequence[0]) | (sink == sequence[0]) | (tallies[sink] == 0), 0, jnp.maximum(margin, 0))
    passed = jax.random.randint(jax.random.fold_in(own, 4), (number_of // 2,), 0, 1 << 20) % (margin + 1)
    tallies = tallies.at[giver].add(-passed).at[sink].add(passed)
    members = jnp.searchsorted(jnp.cumsum(tallies), jnp.arange(rows * top), side="right").astype(jnp.int32)
    table = members.reshape(top, rows).T
    table = table[jax.random.permutation(jax.random.fold_in(own, 1), rows)]
    offset_by = jax.random.randint(jax.random.fold_in(own, 2), (rows, 1), 0, top)
    return jnp.take_along_axis(table, (jnp.arange(top)[None, :] + offset_by) % top, axis=1)


def portions_of(number_of, total, limit, slope, full):
    loads = [(1 << 20) // math.isqrt(grade ** slope) + 1 for grade in range(1, number_of + 1)]
    largest = limit if full else min(limit, max(-(-total // number_of), total * loads[0] // sum(loads)))
    least = 1 if total - largest >= number_of - 1 else 0
    holding, spare = [largest] + [least] * (number_of - 1), total - largest - least * (number_of - 1)
    while spare > 0:
        movable = [i for i in range(1, number_of) if holding[i] < largest] or [i for i in range(1, number_of) if holding[i] < limit]
        whole, remaining = sum([loads[i] for i in movable]), spare
        for i in movable:
            extra = min(limit - holding[i], max(1, remaining * loads[i] // whole), spare)
            holding[i] = holding[i] + extra
            spare = spare - extra
    return np.array(holding)


def noise(rng, dims, spread, limit, pieces=(), kind=jnp.bfloat16):
    entries = spread * jax.random.normal(rng, dims, jnp.float32)
    if pieces:
        entries = entries * block_levels(rng, dims, pieces, -0.22, 0.18)
    return jnp.clip(entries, -limit, limit).astype(kind)


def setup_inputs(seed: int = 0) -> dict:
    seeds = jax.random.split(jax.random.key(seed), 10)
    prior_ensemble = noise(seeds[0], (ENSEMBLE_SIZE, PROGNOSTIC_VARS, NORTH_SOUTH_SPAN, EAST_WEST_SPAN), 1.0, 6.0, ((0, 16), (2, 16)), jnp.float32)
    spreading_factor = jnp.clip(jnp.exp(jax.random.uniform(seeds[1], (PROGNOSTIC_VARS,), jnp.float32, math.log(0.05), math.log(0.24))), 0.05, 0.24)
    tendency_matrix = noise(seeds[2], (PROGNOSTIC_VARS, PROGNOSTIC_VARS), 0.15, 0.6, (), jnp.float32)
    measured_data = noise(seeds[3], (N_DOM, OBS_TILE), 1.0, 6.0, ((0, 16), (1, 16)), jnp.float32)
    inverse_error = jnp.clip(jnp.exp(math.log(1.0) - 2.3025851 * jax.random.uniform(seeds[4], (N_DOM, OBS_TILE), jnp.float32) ** block_levels(seeds[4], (N_DOM, OBS_TILE), ((0, 16), (1, 16)), -0.2, 0.2)), 0.1, 1.0)
    assigned_subregion_keys = jax.random.split(jax.random.fold_in(seeds[5], 1), N_DOM * OBS_TILE // OBS_DEV)
    assigned_subregion_turns = jax.random.permutation(jax.random.fold_in(seeds[5], 3), N_DOM * OBS_TILE // OBS_DEV)
    assigned_subregion = jax.vmap(lambda own, number: deal_out(jax.random.fold_in(seeds[5], 2), own, number, OBS_DEV, PATCH_TILE, 1, OBS_CAP, 2))(assigned_subregion_keys, assigned_subregion_turns).reshape((N_DOM, OBS_TILE, 1))
    measured_entry = plant(jax.random.randint(seeds[6], (N_DOM, OBS_TILE), 0, PROGNOSTIC_VARS * PATCH), jax.random.fold_in(seeds[6], 1), 0, (PROGNOSTIC_VARS * PATCH) - 1).astype(jnp.int32)
    taper_index = plant(jax.random.randint(seeds[7], (N_DOM, OBS_TILE), 0, LOC_LEVELS), jax.random.fold_in(seeds[7], 1), 0, LOC_LEVELS - 1).astype(jnp.int32)
    taper_factors = jnp.clip(jnp.exp(jax.random.uniform(seeds[8], (LOC_LEVELS,), jnp.float32, math.log(0.2), math.log(1.0))), 0.2, 1.0)
    return {"prior_ensemble": prior_ensemble, "spreading_factor": spreading_factor, "tendency_matrix": tendency_matrix, "measured_data": measured_data, "inverse_error": inverse_error, "assigned_subregion": assigned_subregion, "measured_entry": measured_entry, "taper_index": taper_index, "taper_factors": taper_factors}


HIGH = lax.Precision.HIGHEST

def laplacian_update(haloed_ensemble, ensemble, spreading_factor, tendency_matrix):
    subdomain_lines = ensemble.shape[2]
    beside = jnp.pad(ensemble, ((0, 0), (0, 0), (0, 0), (1, 1)))
    laplace = haloed_ensemble[:, :, 2:] + haloed_ensemble[:, :, :subdomain_lines] + beside[:, :, :, 2:] + beside[:, :, :, :-2] - 4.0 * ensemble
    mixing = jnp.einsum('vw,kwxy->kvxy', tendency_matrix, ensemble, precision=HIGH)
    return ensemble + spreading_factor[None, :, None, None] * laplace + mixing

def transforms(gram, drive, member_count):
    identity_m = jnp.eye(member_count, dtype=jnp.float32)
    system = (member_count - 1.0) * identity_m + gram
    norm_value = jnp.sqrt(lax.optimization_barrier(jnp.sum(system * system, axis=(-2, -1))))
    iterate = system / norm_value[..., None, None]
    inverse = jnp.broadcast_to(identity_m, system.shape)
    for sweep_no in range(NS_ITERS):
        middle = 1.5 * identity_m - 0.5 * jnp.einsum('...ij,...jk->...ik', inverse, iterate, precision=HIGH)
        iterate = jnp.einsum('...ij,...jk->...ik', iterate, middle, precision=HIGH)
        inverse = jnp.einsum('...ij,...jk->...ik', middle, inverse, precision=HIGH)
    root = inverse / jnp.sqrt(norm_value)[..., None, None]
    inner = jnp.einsum('...ij,...j->...i', root, drive, precision=HIGH)
    offset = jnp.einsum('...ij,...j->...i', root, inner, precision=HIGH)
    return offset[..., :, None] + jnp.sqrt(member_count - 1.0) * root

def reference(prior_ensemble, spreading_factor, tendency_matrix, measured_data, inverse_error, assigned_subregion, measured_entry, taper_index, taper_factors):
    subdomain_number = prior_ensemble.reshape(ENSEMBLE_SIZE, PROGNOSTIC_VARS, N_DOM, SUBDOMAIN_LINES, EAST_WEST_SPAN)
    blank = jnp.zeros((ENSEMBLE_SIZE, PROGNOSTIC_VARS, 1, EAST_WEST_SPAN), jnp.float32)
    last_rows = subdomain_number[:, :, :, SUBDOMAIN_LINES - 1, :]
    first_rows = subdomain_number[:, :, :, 0, :]
    below_all = jnp.concatenate([blank, last_rows[:, :, :-1]], axis=2)
    above_all = jnp.concatenate([first_rows[:, :, 1:], blank], axis=2)
    weights_all = inverse_error * taper_factors[taper_index]

    def one_tile(tile_index):
        block = lax.dynamic_index_in_dim(subdomain_number, tile_index, 2, keepdims=False)
        below = lax.dynamic_slice_in_dim(below_all, tile_index, 1, 2)
        above = lax.dynamic_slice_in_dim(above_all, tile_index, 1, 2)
        haloed_ensemble = jnp.concatenate([below, block, above], axis=2)
        advanced_ensemble = laplacian_update(haloed_ensemble, block, spreading_factor, tendency_matrix).reshape(ENSEMBLE_SIZE, PROGNOSTIC_VARS, PATCH_TILE, PATCH)
        tile_patch = lax.dynamic_index_in_dim(assigned_subregion, tile_index, 0, keepdims=False)[:, 0]
        tile_cell = lax.dynamic_index_in_dim(measured_entry, tile_index, 0, keepdims=False)
        tile_value = lax.dynamic_index_in_dim(measured_data, tile_index, 0, keepdims=False)
        tile_weight = lax.dynamic_index_in_dim(weights_all, tile_index, 0, keepdims=False)

        def one_patch(patch_index):
            ensemble = lax.dynamic_index_in_dim(advanced_ensemble, patch_index, 2, keepdims=False).reshape(ENSEMBLE_SIZE, PROGNOSTIC_VARS * PATCH)
            centre = lax.optimization_barrier(jnp.mean(ensemble, axis=0))
            deviation = ensemble - centre[None]
            chosen = jnp.where(tile_patch == patch_index, tile_weight, jnp.zeros_like(tile_weight))
            columns = jnp.take(deviation, tile_cell, axis=1)
            innovation = tile_value - jnp.take(centre, tile_cell)
            weighted = columns * chosen[None]
            gram = jnp.dot(weighted, columns.T, precision=HIGH)
            drive = jnp.dot(weighted, innovation, precision=HIGH)
            coeffs = transforms(gram, drive, ENSEMBLE_SIZE)
            return centre[None] + jnp.dot(coeffs.T, deviation, precision=HIGH)
        done = lax.map(one_patch, jnp.arange(PATCH_TILE, dtype=jnp.int32))
        return done.reshape(PATCH_TILE, ENSEMBLE_SIZE, PROGNOSTIC_VARS, PATCH).transpose(1, 2, 0, 3).reshape(ENSEMBLE_SIZE, PROGNOSTIC_VARS, SUBDOMAIN_LINES, EAST_WEST_SPAN)
    result = lax.map(one_tile, jnp.arange(N_DOM, dtype=jnp.int32))
    return result.transpose(1, 2, 0, 3, 4).reshape(ENSEMBLE_SIZE, PROGNOSTIC_VARS, N_DOM * SUBDOMAIN_LINES, EAST_WEST_SPAN)
```

```python
import functools

import jax
import jax.numpy as jnp
from jax import lax
from jax.experimental import pallas as pl
from jax.experimental.pallas import tpu as pltpu
from jax.sharding import PartitionSpec as P


F32 = jnp.float32
BF16 = jnp.bfloat16
HIGH = lax.Precision.HIGHEST
NS_ITERS = 5
CHIPS = 8
SHARE = 4
VARS = 4
LINES = 128
WIDTH = 512
HALF = 32
CAP = 32
OBS = 512
BLOCK = SHARE * VARS * 4 * 8
MB = 1 << 20


def params(mib):
    return pltpu.CompilerParams(vmem_limit_bytes=mib * MB)


def vmem():
    return pl.BlockSpec(memory_space=pltpu.VMEM)


def smem():
    return pl.BlockSpec(memory_space=pltpu.SMEM)


def after():
    return pl.BlockSpec(memory_space=pl.ANY)


def base_row(chunk, chip):
    if chunk == 0:
        return 32 + 8 * chip
    return 8 * chip + jnp.where(chip >= 4, 64, 0)


def stencil_kernel(chunk, place, spread, mix, *refs):
    if chunk == 1:
        _, low, high, x, *outs = refs
    else:
        x, *outs, first, last = refs
        for v in range(VARS):
            first[0, v] = x[0, v, 0:1, :]
            last[0, v] = x[0, v, LINES - 1 : LINES, :]
    chip, core = place[0], place[1]
    row = lax.broadcasted_iota(jnp.int32, (8, WIDTH), 0)
    lane = lax.broadcasted_iota(jnp.int32, (8, WIDTH), 1)
    for d in range(CHIPS):
        target = lax.rem(chip + d, CHIPS)
        base = pl.multiple_of(base_row(chunk, target), 8)
        if chunk == 0:
            before = pl.multiple_of(base - 8, 8)
            behind = pl.multiple_of(base + 8, 8)
        else:
            before = pl.multiple_of(jnp.maximum(base - 8, 0), 8)
            behind = pl.multiple_of(jnp.minimum(base + 8, LINES - 8), 8)
        tiles = [x[0, v, pl.ds(base, 8), :] for v in range(VARS)]
        for v in range(VARS):
            t = tiles[v]
            prev = pltpu.roll(x[0, v, pl.ds(before, 8), :], 1, 0)
            nxt = pltpu.roll(x[0, v, pl.ds(behind, 8), :], 7, 0)
            if chunk == 1:
                prev = jnp.where(base == 0, jnp.broadcast_to(low[0, v], (8, WIDTH)), prev)
                nxt = jnp.where(base == LINES - 8, jnp.broadcast_to(high[0, v], (8, WIDTH)), nxt)
            up = jnp.where(row == 0, prev, pltpu.roll(t, 1, 0))
            down = jnp.where(row == 7, nxt, pltpu.roll(t, 7, 0))
            left = jnp.where(lane == 0, 0.0, pltpu.roll(t, 1, 1))
            right = jnp.where(lane == WIDTH - 1, 0.0, pltpu.roll(t, WIDTH - 1, 1))
            laplace = down + up + right + left - 4.0 * t
            mixing = mix[v, 0] * tiles[0]
            for w in range(1, VARS):
                mixing = mixing + mix[v, w] * tiles[w]
            res = t + spread[v] * laplace + mixing
            res = jnp.where(core == 1, pltpu.roll(res, 4, 0), res)
            for q in range(4):
                outs[d][pl.ds((v * 4 + q) * 8, 8), :] = res[:, q * 128 : (q + 1) * 128]


def stencil(chunk, place, spread, mix, x, extra):
    per = BLOCK // SHARE
    halo_spec = pl.BlockSpec((1, VARS, 1, WIDTH), lambda m: (m, 0, 0, 0))
    out_specs = [pl.BlockSpec((per, 128), lambda m: (m, 0))] * CHIPS
    out_shape = [jax.ShapeDtypeStruct((BLOCK, 128), F32)] * CHIPS
    extra_specs = [after(), halo_spec, halo_spec]
    if chunk == 0:
        out_specs += [halo_spec] * 2
        out_shape += [jax.ShapeDtypeStruct((SHARE, VARS, 1, WIDTH), F32)] * 2
        extra_specs = []
    return pl.pallas_call(
        functools.partial(stencil_kernel, chunk),
        grid=(SHARE,),
        in_specs=[smem(), smem(), smem()]
        + extra_specs
        + [pl.BlockSpec((1, VARS, LINES, WIDTH), lambda m: (m, 0, 0, 0))],
        out_specs=out_specs,
        out_shape=out_shape,
        compiler_params=params(16),
        cost_estimate=pl.CostEstimate(flops=20_000_000, bytes_accessed=6 * MB, transcendentals=0),
    )(place, spread, mix, *extra, x)


def parts3(x):
    a = x.astype(BF16)
    r = x - a.astype(F32)
    b = r.astype(BF16)
    c = (r - b.astype(F32)).astype(BF16)
    return a, b, c


def nt(a, b):
    return lax.dot_general(a, b, (((1,), (1,)), ((), ())), preferred_element_type=F32)


def obs_kernel(_, pid, tidx, entry, value, inv, table, out):
    ids = pid[...]
    sub = lax.broadcasted_iota(jnp.int32, (32, OBS), 0)
    named = sub == jnp.broadcast_to(ids, (32, OBS))
    onehot = jnp.where(named, 1.0, 0.0)
    earlier = jnp.where(
        lax.broadcasted_iota(jnp.int32, (OBS, OBS), 0) < lax.broadcasted_iota(jnp.int32, (OBS, OBS), 1),
        1.0, 0.0,
    ).astype(BF16)
    before = jnp.dot(onehot.astype(BF16), earlier, preferred_element_type=F32)
    rank = jnp.sum(before * onehot, axis=0, keepdims=True).astype(jnp.int32)
    inner = (ids >= 8) & (ids < 24)
    group = jnp.where(inner, 2 * (ids - 8), jnp.where(ids < 8, 2 * ids + 1, 2 * (ids - 16) + 1))
    target = group * CAP + rank
    levels = table.shape[1]
    look = jnp.where(
        lax.broadcasted_iota(jnp.int32, (levels, OBS), 0) == jnp.broadcast_to(tidx[...], (levels, OBS)),
        1.0, 0.0,
    ).astype(BF16)
    taper = sum(
        jnp.dot(jnp.broadcast_to(p, (16, levels)), look, preferred_element_type=F32)
        for p in parts3(table[...])
    )
    weight = inv[...] * taper[0:1]
    c = entry[...]
    place = (c & 0x1800) | ((c & 0x180) << 2) | ((c & 0x600) >> 2) | (c & 0x7F)
    r8 = lax.broadcasted_iota(jnp.int32, (16, OBS), 0)
    fields = jnp.where(
        r8 == 0, jnp.broadcast_to(value[...], (16, OBS)),
        jnp.where(r8 == 1, jnp.broadcast_to(weight, (16, OBS)),
                  jnp.where(r8 == 2, jnp.broadcast_to(place.astype(F32), (16, OBS)), 0.0)),
    )
    pieces = parts3(fields)
    for k in range(2):
        slots = jnp.where(
            lax.broadcasted_iota(jnp.int32, (OBS, OBS), 0) + k * OBS == jnp.broadcast_to(target, (OBS, OBS)),
            1.0, 0.0,
        ).astype(BF16)
        placed = nt(pieces[0], slots) + nt(pieces[1], slots) + nt(pieces[2], slots)
        out[:, pl.ds(k * OBS, OBS)] = placed[0:8]


def place_obs(behind, pid, tidx, entry, value, inv, table):
    return pl.pallas_call(
        obs_kernel,
        in_specs=[after()] + [vmem()] * 6,
        out_specs=vmem(),
        out_shape=jax.ShapeDtypeStruct((8, 2 * OBS), F32),
        compiler_params=params(16),
        cost_estimate=pl.CostEstimate(flops=20_000_000, bytes_accessed=MB, transcendentals=0),
        name="place_obs",
    )(behind, pid, tidx, entry, value, inv, table)


def gather_members_kernel(_, *refs):
    blocks, (keep, send) = refs[:CHIPS], refs[CHIPS:]
    for g in range(64):
        vl, r = g // 4, g % 4
        for d in range(CHIPS):
            keep[g, pl.ds(SHARE * d, SHARE), :] = blocks[d][pl.ds(vl * 8 + r, SHARE, stride=128), :]
            send[g, pl.ds(SHARE * d, SHARE), :] = blocks[d][pl.ds(vl * 8 + 4 + r, SHARE, stride=128), :]


def gather_members(behind, blocks):
    half = jax.ShapeDtypeStruct((64, HALF, 128), F32)
    return pl.pallas_call(
        gather_members_kernel,
        in_specs=[after()] + [vmem()] * CHIPS,
        out_specs=[vmem()] * 2,
        out_shape=[half] * 2,
        compiler_params=params(16),
        cost_estimate=pl.CostEstimate(flops=20_000_000, bytes_accessed=4 * MB, transcendentals=0),
    )(behind, *blocks)


def spread_members_kernel(keep, came, *outs):
    for d in range(CHIPS):
        for m in range(SHARE):
            for vl in range(16):
                at = (m * 16 + vl) * 8
                start = vl * 128 + d * SHARE + m
                outs[d][pl.ds(at, 4), :] = keep[pl.ds(start, 4, stride=HALF), :]
                outs[d][pl.ds(at + 4, 4), :] = came[pl.ds(start, 4, stride=HALF), :]


def spread_members(keep, came):
    return pl.pallas_call(
        spread_members_kernel,
        in_specs=[vmem()] * 2,
        out_specs=[vmem()] * CHIPS,
        out_shape=[jax.ShapeDtypeStruct((BLOCK, 128), F32)] * CHIPS,
        compiler_params=params(16),
        cost_estimate=pl.CostEstimate(flops=20_000_000, bytes_accessed=4 * MB, transcendentals=0),
    )(keep.reshape(64 * HALF, 128), came.reshape(64 * HALF, 128))


def high(a, b):
    return jnp.dot(a, b, precision=HIGH, preferred_element_type=F32)


def analysis_kernel(keep, came, obs, out_keep, out_send, parts, centres, acc):
    members = 2 * HALF
    acc[...] = jnp.zeros_like(acc)
    cell = lax.broadcasted_iota(jnp.int32, (256, OBS), 0)
    where_obs = obs[2:3, :].astype(jnp.int32)

    def select(t, _):
        g = 2 * t
        cols = [jnp.concatenate([keep[g + h], came[g + h]], axis=0) for h in range(2)]
        block = jnp.concatenate(cols, axis=1)
        centre = jnp.sum(block, axis=0, keepdims=True) * (1.0 / members)
        dev = block - centre
        hi = dev.astype(BF16)
        lo = (dev - hi.astype(F32)).astype(BF16)
        c1 = centre.astype(BF16)
        rest = centre - c1.astype(F32)
        c2 = rest.astype(BF16)
        c3 = rest - c2.astype(F32)
        row = lax.broadcasted_iota(jnp.int32, (16, 256), 0)
        crows = jnp.where(
            row == 0, jnp.broadcast_to(c1.astype(F32), (16, 256)),
            jnp.where(row == 1, jnp.broadcast_to(c2.astype(F32), (16, 256)),
                      jnp.where(row == 2, jnp.broadcast_to(c3, (16, 256)), 0.0)),
        ).astype(BF16)
        both = jnp.concatenate([hi, lo], axis=0)
        parts[t] = both
        centres[t] = jnp.broadcast_to(centre, (8, 256))
        chosen = jnp.where(cell == jnp.broadcast_to(where_obs - t * 256, (256, OBS)), 1.0, 0.0).astype(BF16)
        acc[...] += jnp.dot(jnp.concatenate([both, crows], axis=0), chosen, preferred_element_type=F32)
        return 0

    lax.fori_loop(0, 32, select, 0)
    columns = acc[0:members] + acc[members : 2 * members]
    centre_obs = acc[128:129] + acc[129:130] + acc[130:131]
    innovation = obs[0:1, :] - centre_obs
    weight = obs[1:2, :]
    weighted = columns * weight
    pair = (((1,), (1,)), ((), ()))
    gram = lax.dot_general(weighted, columns, pair, precision=HIGH, preferred_element_type=F32)
    drive = lax.dot_general(
        jnp.broadcast_to(weight * innovation, (8, OBS)), columns, pair, precision=HIGH, preferred_element_type=F32
    )
    eye = jnp.where(
        lax.broadcasted_iota(jnp.int32, (members, members), 0) == lax.broadcasted_iota(jnp.int32, (members, members), 1),
        1.0, 0.0,
    )
    system = (members - 1.0) * eye + gram
    norm = jnp.sqrt(jnp.sum(jnp.sum(system * system, axis=1, keepdims=True), axis=0, keepdims=True))
    y = system / norm
    z = 1.5 * eye - 0.5 * y
    y = high(y, z)
    for sweep in range(1, NS_ITERS):
        mid = 1.5 * eye - 0.5 * high(z, y)
        if sweep < NS_ITERS - 1:
            y = high(y, mid)
        z = high(mid, z)
    root = z / jnp.sqrt(norm)
    offset = high(high(drive, root), root)
    coeff = offset[0:1, :] + jnp.sqrt(members - 1.0) * root
    spread = jnp.where(
        lax.broadcasted_iota(jnp.int32, (members, 256), 0)
        == (lax.broadcasted_iota(jnp.int32, (members, 256), 1) & (members - 1)),
        1.0, 0.0,
    )
    four = high(coeff, spread)
    four_hi = four.astype(BF16)
    four_lo = four - four_hi.astype(F32)
    lanes = lax.broadcasted_iota(jnp.int32, (members, 256), 1)
    left = jnp.where(lanes < 128, four_hi.astype(F32), four_lo).astype(BF16)

    def transform(t, _):
        g = 2 * t
        both = parts[t]
        res = jnp.dot(left, jnp.concatenate([both, both], axis=0), preferred_element_type=F32)
        res = res + jnp.broadcast_to(centres[t][0:1], (members, 256))
        for h in range(2):
            out_keep[g + h] = res[0:HALF, h * 128 : (h + 1) * 128]
            out_send[g + h] = res[HALF:members, h * 128 : (h + 1) * 128]
        return 0

    lax.fori_loop(0, 32, transform, 0)


def analysis(keep, came, obs):
    half = jax.ShapeDtypeStruct((64, HALF, 128), F32)
    return pl.pallas_call(
        analysis_kernel,
        in_specs=[vmem()] * 3,
        out_specs=[vmem()] * 2,
        out_shape=[half] * 2,
        scratch_shapes=[
            pltpu.VMEM((32, 128, 256), BF16),
            pltpu.VMEM((32, 8, 256), F32),
            pltpu.VMEM((144, OBS), F32),
        ],
        compiler_params=params(24),
        cost_estimate=pl.CostEstimate(flops=100_000_000, bytes_accessed=4 * MB, transcendentals=0),
    )(keep, came, obs)


def grid_kernel(place, *refs):
    blocks, out = refs[:-1], refs[-1]
    chip, core = place[0], place[1]
    for chunk in range(2):
        for d in range(CHIPS):
            base = pl.multiple_of(base_row(chunk, lax.rem(chip + d, CHIPS)), 8)
            src = blocks[chunk * CHIPS + d]
            for v in range(VARS):
                for q in range(4):
                    val = src[pl.ds((v * 4 + q) * 8, 8), :]
                    val = jnp.where(core == 1, pltpu.roll(val, 4, 0), val)
                    out[0, v, pl.ds(base, 8), q * 128 : (q + 1) * 128] = val


def to_grid(place, blocks):
    per = BLOCK // SHARE
    return pl.pallas_call(
        grid_kernel,
        grid=(SHARE,),
        in_specs=[smem()] + [pl.BlockSpec((per, 128), lambda m: (m, 0))] * (2 * CHIPS),
        out_specs=pl.BlockSpec((1, VARS, LINES, WIDTH), lambda m: (m, 0, 0, 0)),
        out_shape=jax.ShapeDtypeStruct((SHARE, VARS, LINES, WIDTH), F32),
        compiler_params=params(16),
        cost_estimate=pl.CostEstimate(flops=5_000_000, bytes_accessed=8 * MB, transcendentals=0),
        name="to_grid",
    )(place, *blocks)


def hop(block, d):
    n = 2 * CHIPS
    return lax.ppermute(block, "mem", [(i, (i + 2 * d) % n) for i in range(n)])


ORDER = (4, 3, 5, 2, 6, 1, 7)


def exchange(blocks, sign):
    got = list(blocks)
    for d in ORDER:
        got[d] = hop(blocks[d], sign * d)
    return got


def swap(x):
    return lax.ppermute(x, "mem", [(i, i ^ 1) for i in range(2 * CHIPS)])


def shards(
    prior_ensemble,
    spreading_factor,
    tendency_matrix,
    measured_data,
    inverse_error,
    assigned_subregion,
    measured_entry,
    taper_index,
    taper_factors,
):
    me = lax.axis_index("mem")
    place = jnp.stack([me // 2, me % 2]).astype(jnp.int32)
    x = prior_ensemble

    *sent_a, first, last = stencil(0, place, spreading_factor, tendency_matrix, x, ())
    got_a = exchange(sent_a, 1)

    placed = place_obs(
        sent_a[0], assigned_subregion.reshape(1, OBS), taper_index, measured_entry, measured_data,
        inverse_error, taper_factors.reshape(1, -1),
    )
    outgoing = placed[0:3].reshape(3, 16, 64).transpose(1, 0, 2).reshape(16, 192)
    incoming = lax.all_to_all(outgoing, "mem", split_axis=0, concat_axis=0, tiled=True)
    slots = incoming.reshape(16, 3, 2, CAP).transpose(2, 1, 0, 3).reshape(2, 3, OBS)
    slots = jnp.pad(slots, ((0, 0), (0, 5), (0, 0)))

    count = lax.axis_size("dom")
    forward = [(i, i + 1) for i in range(count - 1)]
    backward = [(b, a) for a, b in forward]
    low = lax.ppermute(last, "dom", forward)
    high_row = lax.ppermute(first, "dom", backward)
    sent_b = stencil(1, place, spreading_factor, tendency_matrix, x, (placed, low, high_row))
    got_b = exchange(sent_b, 1)

    back = []
    behind = sent_b[0]
    for chunk, got in enumerate((got_a, got_b)):
        keep, send = gather_members(behind, got)
        came = swap(send)
        out_keep, out_send = analysis(keep, came, slots[chunk])
        returned = swap(out_send)
        outs = spread_members(out_keep, returned)
        back.extend(exchange(outs, -1))
        behind = outs[0]
    return to_grid(place, back)


def solution(mesh):
    in_specs = (
        P("mem", None, "dom", None),
        P(),
        P(),
        P("dom", "mem"),
        P("dom", "mem"),
        P("dom", "mem", None),
        P("dom", "mem"),
        P("dom", "mem"),
        P(),
    )
    out_specs = P("mem", None, "dom", None)

    return jax.shard_map(shards, mesh=mesh, in_specs=in_specs, out_specs=out_specs, check_vma=False)
```

```python
import functools

import jax
import jax.numpy as jnp
from jax import lax
from jax.experimental import pallas as pl
from jax.experimental.pallas import tpu as pltpu
from jax.sharding import PartitionSpec as P


F32 = jnp.float32
BF16 = jnp.bfloat16
HIGH = lax.Precision.HIGHEST
NS_ITERS = 5
CHIPS = 8
SHARE = 4
VARS = 4
LINES = 128
WIDTH = 512
HALF = 32
CAP = 32
OBS = 512
BLOCK = SHARE * VARS * 4 * 8
MB = 1 << 20


ALL_VMEM = 67_043_328


def params(mib=None):
    return pltpu.CompilerParams(vmem_limit_bytes=ALL_VMEM if mib is None else mib * MB)


def vmem():
    return pl.BlockSpec(memory_space=pltpu.VMEM)


def base_row(chunk, chip):
    if chunk == 0:
        return 32 + 8 * chip
    return 8 * chip + jnp.where(chip >= 4, 64, 0)


def stencil_kernel(chunk, dists, part, *refs):
    low = high = obs_in = placed = None
    if part == "first":
        *obs_in, spread_in, mix_in, x = refs[:9]
        refs = refs[9:]
    elif part == "b":
        low, high, spread_in, mix_in, x = refs[:5]
        refs = refs[5:]
    else:
        placed, spread_in, mix_in, x = refs[:4]
        refs = refs[4:]
    outs, refs = refs[: len(dists)], refs[len(dists) :]
    if part == "first":
        placed, *refs = refs
    if part == "rest":
        first_out, last_out, *refs = refs
    win, spread, mix, sems, scalar_sems = refs
    chip = lax.axis_index("mem") // 2
    bases, starts, copies = [], [], []
    for k, d in enumerate(dists):
        base = pl.multiple_of(base_row(chunk, lax.rem(chip + d, CHIPS)), 8)
        start = base - 8 if chunk == 0 else jnp.clip(base - 8, 0, LINES - 24)
        start = pl.multiple_of(start, 8)
        copy = pltpu.make_async_copy(x.at[:, :, pl.ds(start, 24), :], win.at[k], sems.at[k])
        copy.start()
        bases.append(base)
        starts.append(start)
        copies.append(copy)
    scalars = [
        pltpu.make_async_copy(spread_in, spread, scalar_sems.at[0]),
        pltpu.make_async_copy(mix_in, mix, scalar_sems.at[1]),
    ]
    for copy in scalars:
        copy.start()
    edges = []
    if part == "rest":
        edges = [
            pltpu.make_async_copy(x.at[:, :, pl.ds(0, 8), :], first_out, sems.at[len(dists)]),
            pltpu.make_async_copy(x.at[:, :, pl.ds(LINES - 8, 8), :], last_out, sems.at[len(dists) + 1]),
        ]
        for copy in edges:
            copy.start()
    row = lax.broadcasted_iota(jnp.int32, (8, WIDTH), 0)
    lane = lax.broadcasted_iota(jnp.int32, (8, WIDTH), 1)
    if part == "first":
        placed[...] = place_obs(*obs_in)
    if chunk == 0:
        for k, d in enumerate(dists):
            lanes = pl.multiple_of(lax.rem(chip + d, CHIPS) * 128, 128)
            outs[k][BLOCK : BLOCK + 8, :] = placed[:, pl.ds(lanes, 128)]
    for copy in scalars:
        copy.wait()
    for k in range(len(dists)):
        base, out = bases[k], outs[k]
        copies[k].wait()
        if chunk == 0:
            here, before, behind = 8, 0, 16
        else:
            here = pl.multiple_of(base - starts[k], 8)
            before = pl.multiple_of(jnp.maximum(here - 8, 0), 8)
            behind = pl.multiple_of(jnp.minimum(here + 8, 16), 8)

        def member(m, _, k=k, base=base, out=out, here=here, before=before, behind=behind):
            tiles = [win[k, m, v, pl.ds(here, 8), :] for v in range(VARS)]
            for v in range(VARS):
                t = tiles[v]
                prev = pltpu.roll(win[k, m, v, pl.ds(before, 8), :], 1, 0)
                nxt = pltpu.roll(win[k, m, v, pl.ds(behind, 8), :], 7, 0)
                if chunk == 1:
                    prev = jnp.where(base == 0, pltpu.roll(low[m, v], 1, 0), prev)
                    nxt = jnp.where(base == LINES - 8, pltpu.roll(high[m, v], 7, 0), nxt)
                up = jnp.where(row == 0, prev, pltpu.roll(t, 1, 0))
                down = jnp.where(row == 7, nxt, pltpu.roll(t, 7, 0))
                left = jnp.where(lane == 0, 0.0, pltpu.roll(t, 1, 1))
                right = jnp.where(lane == WIDTH - 1, 0.0, pltpu.roll(t, WIDTH - 1, 1))
                laplace = down + up + right + left - 4.0 * t
                mixing = mix[v, 0] * tiles[0]
                for w in range(1, VARS):
                    mixing = mixing + mix[v, w] * tiles[w]
                res = t + spread[v] * laplace + mixing
                for q in range(4):
                    at = pl.multiple_of(m * 128 + (v * 4 + q) * 8, 8)
                    out[pl.ds(at, 8), :] = res[:, q * 128 : (q + 1) * 128]
            return 0

        lax.fori_loop(0, SHARE, member, 0)
    for copy in edges:
        copy.wait()


def hbm():
    return pl.BlockSpec(memory_space=pltpu.HBM)


def stencil(chunk, dists, part, extra, spread, mix, x):
    n = len(dists)
    rows = BLOCK + 8 if chunk == 0 else BLOCK
    more = []
    if part == "first":
        more = [jax.ShapeDtypeStruct((8, 2 * OBS), F32)]
    if part == "rest":
        more = [jax.ShapeDtypeStruct((SHARE, VARS, 8, WIDTH), F32)] * 2
    res = pl.pallas_call(
        functools.partial(stencil_kernel, chunk, dists, part),
        in_specs=[vmem()] * len(extra) + [hbm()] * 3,
        out_specs=[vmem()] * (n + len(more)),
        out_shape=[jax.ShapeDtypeStruct((rows, 128), F32)] * n + more,
        scratch_shapes=[
            pltpu.VMEM((n, SHARE, VARS, 24, WIDTH), F32),
            pltpu.SMEM((VARS,), F32),
            pltpu.SMEM((VARS, VARS), F32),
            pltpu.SemaphoreType.DMA((n + 2,)),
            pltpu.SemaphoreType.DMA((2,)),
        ],
        compiler_params=params(),
        cost_estimate=pl.CostEstimate(flops=2_500_000 * n, bytes_accessed=n * MB, transcendentals=0),
    )(*extra, spread, mix, x)
    return dict(zip(dists, res[:n])), res[n:]


def parts3(x):
    a = x.astype(BF16)
    r = x - a.astype(F32)
    b = r.astype(BF16)
    c = (r - b.astype(F32)).astype(BF16)
    return a, b, c


def nt(a, b):
    return lax.dot_general(a, b, (((1,), (1,)), ((), ())), preferred_element_type=F32)


def place_obs(pid, tidx, entry, value, inv, table):
    ids = pid[...]
    sub = lax.broadcasted_iota(jnp.int32, (32, OBS), 0)
    named = sub == jnp.broadcast_to(ids, (32, OBS))
    onehot = jnp.where(named, 1.0, 0.0)
    earlier = jnp.where(
        lax.broadcasted_iota(jnp.int32, (OBS, OBS), 0) < lax.broadcasted_iota(jnp.int32, (OBS, OBS), 1),
        1.0, 0.0,
    ).astype(BF16)
    before = jnp.dot(onehot.astype(BF16), earlier, preferred_element_type=F32)
    rank = jnp.sum(before * onehot, axis=0, keepdims=True).astype(jnp.int32)
    inner = (ids >= 8) & (ids < 24)
    group = jnp.where(inner, 2 * (ids - 8), jnp.where(ids < 8, 2 * ids + 1, 2 * (ids - 16) + 1))
    target = group * CAP + rank
    levels = table.shape[1]
    look = jnp.where(
        lax.broadcasted_iota(jnp.int32, (levels, OBS), 0) == jnp.broadcast_to(tidx[...], (levels, OBS)),
        1.0, 0.0,
    ).astype(BF16)
    taper = sum(
        jnp.dot(jnp.broadcast_to(p, (16, levels)), look, preferred_element_type=F32)
        for p in parts3(table[...])
    )
    weight = inv[...] * taper[0:1]
    c = entry[...]
    place = (c & 0x1800) | ((c & 0x180) << 2) | ((c & 0x600) >> 2) | (c & 0x7F)
    r8 = lax.broadcasted_iota(jnp.int32, (16, OBS), 0)
    fields = jnp.where(
        r8 == 0, jnp.broadcast_to(value[...], (16, OBS)),
        jnp.where(r8 == 1, jnp.broadcast_to(weight, (16, OBS)),
                  jnp.where(r8 == 2, jnp.broadcast_to(place.astype(F32), (16, OBS)), 0.0)),
    )
    pieces = parts3(fields)
    halves = []
    for k in range(2):
        slots = jnp.where(
            lax.broadcasted_iota(jnp.int32, (OBS, OBS), 0) + k * OBS == jnp.broadcast_to(target, (OBS, OBS)),
            1.0, 0.0,
        ).astype(BF16)
        placed = nt(pieces[0], slots) + nt(pieces[1], slots) + nt(pieces[2], slots)
        halves.append(placed[0:8])
    return jnp.concatenate(halves, axis=1)


def gather_members_kernel(chunk, *refs):
    blocks, (keep, send) = refs[:CHIPS], refs[CHIPS:]
    core = lax.axis_index("mem") % 2
    own = 4 * core
    for g in range(64):
        vl, r = g // 4, g % 4
        for d in range(CHIPS):
            keep[g, pl.ds(SHARE * d, SHARE), :] = blocks[d][pl.ds(vl * 8 + r + own, SHARE, stride=128), :]
            send[g, pl.ds(SHARE * d, SHARE), :] = blocks[d][pl.ds(vl * 8 + r + 4 - own, SHARE, stride=128), :]
    if chunk == 0:
        quarter = lax.broadcasted_iota(jnp.int32, (8, 128), 1) // CAP
        for out, whose in ((keep, core), (send, 1 - core)):
            for q in range(4):
                first = whose * 64 + (q // 2) * CAP
                packed = jnp.zeros((8, 128), F32)
                for k in range(4):
                    tile = blocks[(q % 2) * 4 + k][BLOCK : BLOCK + 8, :]
                    moved = pltpu.roll(tile, (k * CAP - first) & 127, 1)
                    packed = jnp.where(quarter == k, moved, packed)
                out[64, pl.ds(q * 8, 8), :] = packed


def gather_members(chunk, blocks):
    half = jax.ShapeDtypeStruct((65 if chunk == 0 else 64, HALF, 128), F32)
    return pl.pallas_call(
        functools.partial(gather_members_kernel, chunk),
        in_specs=[vmem()] * CHIPS,
        out_specs=[vmem()] * 2,
        out_shape=[half] * 2,
        compiler_params=params(16),
        cost_estimate=pl.CostEstimate(flops=20_000_000, bytes_accessed=4 * MB, transcendentals=0),
    )(*blocks)


def spread_members_kernel(keep, came, *outs):
    own = 4 * (lax.axis_index("mem") % 2)
    for d in range(CHIPS):
        for m in range(SHARE):
            for vl in range(16):
                at = (m * 16 + vl) * 8
                start = vl * 128 + d * SHARE + m
                outs[d][pl.ds(at + own, 4), :] = keep[pl.ds(start, 4, stride=HALF), :]
                outs[d][pl.ds(at + 4 - own, 4), :] = came[pl.ds(start, 4, stride=HALF), :]


def spread_members(keep, came):
    return pl.pallas_call(
        spread_members_kernel,
        in_specs=[vmem()] * 2,
        out_specs=[vmem()] * CHIPS,
        out_shape=[jax.ShapeDtypeStruct((BLOCK, 128), F32)] * CHIPS,
        compiler_params=params(16),
        cost_estimate=pl.CostEstimate(flops=20_000_000, bytes_accessed=4 * MB, transcendentals=0),
    )(keep.reshape(64 * HALF, 128), came.reshape(64 * HALF, 128))


def high(a, b):
    return jnp.dot(a, b, precision=HIGH, preferred_element_type=F32)


def analysis_kernel(chunk, keep, came, *refs):
    if chunk == 0:
        out_keep, out_send, later, parts, centres, acc = refs
        tiles = [[half[64, q * 8 : (q + 1) * 8, :] for half in (keep, came) for q in pair] for pair in ((0, 1), (2, 3))]
        obs = jnp.concatenate(tiles[0], axis=1)
        later[...] = jnp.concatenate(tiles[1], axis=1)
    else:
        obs_in, out_keep, out_send, parts, centres, acc = refs
        obs = obs_in[...]
    members = 2 * HALF
    acc[...] = jnp.zeros_like(acc)
    cell = lax.broadcasted_iota(jnp.int32, (256, OBS), 0)
    where_obs = obs[2:3, :].astype(jnp.int32)

    def select(t, _):
        g = 2 * t
        cols = [jnp.concatenate([keep[g + h], came[g + h]], axis=0) for h in range(2)]
        block = jnp.concatenate(cols, axis=1)
        centre = jnp.sum(block, axis=0, keepdims=True) * (1.0 / members)
        dev = block - centre
        hi = dev.astype(BF16)
        lo = (dev - hi.astype(F32)).astype(BF16)
        c1 = centre.astype(BF16)
        rest = centre - c1.astype(F32)
        c2 = rest.astype(BF16)
        c3 = rest - c2.astype(F32)
        row = lax.broadcasted_iota(jnp.int32, (16, 256), 0)
        crows = jnp.where(
            row == 0, jnp.broadcast_to(c1.astype(F32), (16, 256)),
            jnp.where(row == 1, jnp.broadcast_to(c2.astype(F32), (16, 256)),
                      jnp.where(row == 2, jnp.broadcast_to(c3, (16, 256)), 0.0)),
        ).astype(BF16)
        both = jnp.concatenate([hi, lo], axis=0)
        parts[t] = both
        centres[t] = jnp.broadcast_to(centre, (8, 256))
        chosen = jnp.where(cell == jnp.broadcast_to(where_obs - t * 256, (256, OBS)), 1.0, 0.0).astype(BF16)
        acc[...] += jnp.dot(jnp.concatenate([both, crows], axis=0), chosen, preferred_element_type=F32)
        return 0

    lax.fori_loop(0, 32, select, 0)
    columns = acc[0:members] + acc[members : 2 * members]
    centre_obs = acc[128:129] + acc[129:130] + acc[130:131]
    innovation = obs[0:1, :] - centre_obs
    weight = obs[1:2, :]
    weighted = columns * weight
    pair = (((1,), (1,)), ((), ()))
    gram = lax.dot_general(weighted, columns, pair, precision=HIGH, preferred_element_type=F32)
    drive = lax.dot_general(
        jnp.broadcast_to(weight * innovation, (8, OBS)), columns, pair, precision=HIGH, preferred_element_type=F32
    )
    eye = jnp.where(
        lax.broadcasted_iota(jnp.int32, (members, members), 0) == lax.broadcasted_iota(jnp.int32, (members, members), 1),
        1.0, 0.0,
    )
    system = (members - 1.0) * eye + gram
    norm = jnp.sqrt(jnp.sum(jnp.sum(system * system, axis=1, keepdims=True), axis=0, keepdims=True))
    y = system / norm
    z = 1.5 * eye - 0.5 * y
    y = high(y, z)
    for sweep in range(1, NS_ITERS):
        mid = 1.5 * eye - 0.5 * high(z, y)
        if sweep < NS_ITERS - 1:
            y = high(y, mid)
        z = high(mid, z)
    root = z / jnp.sqrt(norm)
    offset = high(high(drive, root), root)
    coeff = offset[0:1, :] + jnp.sqrt(members - 1.0) * root
    spread = jnp.where(
        lax.broadcasted_iota(jnp.int32, (members, 256), 0)
        == (lax.broadcasted_iota(jnp.int32, (members, 256), 1) & (members - 1)),
        1.0, 0.0,
    )
    four = high(coeff, spread)
    four_hi = four.astype(BF16)
    four_lo = four - four_hi.astype(F32)
    lanes = lax.broadcasted_iota(jnp.int32, (members, 256), 1)
    left = jnp.where(lanes < 128, four_hi.astype(F32), four_lo).astype(BF16)

    def transform(t, _):
        g = 2 * t
        both = parts[t]
        res = jnp.dot(left, jnp.concatenate([both, both], axis=0), preferred_element_type=F32)
        res = res + jnp.broadcast_to(centres[t][0:1], (members, 256))
        for h in range(2):
            out_keep[g + h] = res[0:HALF, h * 128 : (h + 1) * 128]
            out_send[g + h] = res[HALF:members, h * 128 : (h + 1) * 128]
        return 0

    lax.fori_loop(0, 32, transform, 0)


def analysis(chunk, keep, came, obs):
    half = jax.ShapeDtypeStruct((64, HALF, 128), F32)
    later = [jax.ShapeDtypeStruct((8, OBS), F32)] if chunk == 0 else []
    return pl.pallas_call(
        functools.partial(analysis_kernel, chunk),
        in_specs=[vmem()] * (2 + len(obs)),
        out_specs=[vmem()] * (2 + len(later)),
        out_shape=[half] * 2 + later,
        scratch_shapes=[
            pltpu.VMEM((32, 128, 256), BF16),
            pltpu.VMEM((32, 8, 256), F32),
            pltpu.VMEM((144, OBS), F32),
        ],
        compiler_params=params(24),
        cost_estimate=pl.CostEstimate(flops=100_000_000, bytes_accessed=4 * MB, transcendentals=0),
    )(keep, came, *obs)


def assemble_kernel(chunk, dists, *refs):
    *refs, out, tiles, sems = refs
    blocks = refs[-len(dists) :]
    chip = lax.axis_index("mem") // 2
    copies = []
    for k, d in enumerate(dists):
        for m in range(SHARE):
            for v in range(VARS):
                for q in range(4):
                    at = (m * 16 + v * 4 + q) * 8
                    tiles[k, m, v, :, q * 128 : (q + 1) * 128] = blocks[k][at : at + 8, :]
        base = pl.multiple_of(base_row(chunk, lax.rem(chip + d, CHIPS)), 8)
        copy = pltpu.make_async_copy(tiles.at[k], out.at[:, :, pl.ds(base, 8), :], sems.at[k])
        copy.start()
        copies.append(copy)
    for copy in copies:
        copy.wait()


def assemble(chunk, dists, grid, blocks):
    n = len(dists)
    kept = [] if grid is None else [grid]
    return pl.pallas_call(
        functools.partial(assemble_kernel, chunk, dists),
        in_specs=[hbm()] * len(kept) + [vmem()] * n,
        out_specs=hbm(),
        out_shape=jax.ShapeDtypeStruct((SHARE, VARS, LINES, WIDTH), F32),
        scratch_shapes=[pltpu.VMEM((n, SHARE, VARS, 8, WIDTH), F32), pltpu.SemaphoreType.DMA((n,))],
        input_output_aliases={0: 0} if kept else {},
        compiler_params=params(8),
        cost_estimate=pl.CostEstimate(flops=1_000_000 * n, bytes_accessed=n * MB // 2, transcendentals=0),
    )(*kept, *[blocks[d] for d in dists])


def hop(block, d):
    n = 2 * CHIPS
    return lax.ppermute(block, "mem", [(i, (i + 2 * d) % n) for i in range(n)])


ORDER = (4, 3, 5, 2, 6, 1, 7)
ALL = ORDER + (0,)
PIECES = ((4, 0, 5), (3, 6, 7), (2, 1))


def exchange(blocks, dists, sign):
    got = {}
    for d in dists:
        if d == 0:
            got[d] = blocks[d]
            continue
        got[d] = hop(blocks[d], sign * d)
    return got


def swap(x):
    return lax.ppermute(x, "mem", [(i, i ^ 1) for i in range(2 * CHIPS)])


def shards(
    prior_ensemble,
    spreading_factor,
    tendency_matrix,
    measured_data,
    inverse_error,
    assigned_subregion,
    measured_entry,
    taper_index,
    taper_factors,
):
    x = prior_ensemble
    physics = (spreading_factor, tendency_matrix, x)

    obs = (
        assigned_subregion.reshape(1, OBS), taper_index, measured_entry, measured_data,
        inverse_error, taper_factors.reshape(1, -1),
    )
    sent, (placed,) = stencil(0, ALL[:1], "first", obs, *physics)
    got_a = exchange(sent, ALL[:1], 1)
    sent, _ = stencil(0, ALL[1:3], "next", (placed,), *physics)
    got_a |= exchange(sent, ALL[1:3], 1)
    sent, (first, last) = stencil(0, ALL[3:], "rest", (placed,), *physics)
    got_a |= exchange(sent, ALL[3:], 1)

    count = lax.axis_size("dom")
    forward = [(i, i + 1) for i in range(count - 1)]
    backward = [(b, a) for a, b in forward]
    low = lax.ppermute(last, "dom", forward)
    high_row = lax.ppermute(first, "dom", backward)
    sent_b, _ = stencil(1, ALL, "b", (low, high_row), *physics)
    got_b = exchange(sent_b, ALL, 1)

    back, slots = [], []
    for chunk, got in enumerate((got_a, got_b)):
        keep, send = gather_members(chunk, [got[d] for d in range(CHIPS)])
        came = swap(send)
        out_keep, out_send, *slots = analysis(chunk, keep, came, slots)
        returned = swap(out_send)
        outs = spread_members(out_keep, returned)
        back.append(exchange(dict(enumerate(outs)), ALL, -1))
    grid = assemble(0, ALL, None, back[0])
    for dists in PIECES:
        grid = assemble(1, dists, grid, back[1])
    return grid


def solution(mesh):
    in_specs = (
        P("mem", None, "dom", None),
        P(),
        P(),
        P("dom", "mem"),
        P("dom", "mem"),
        P("dom", "mem", None),
        P("dom", "mem"),
        P("dom", "mem"),
        P(),
    )
    out_specs = P("mem", None, "dom", None)

    return jax.shard_map(shards, mesh=mesh, in_specs=in_specs, out_specs=out_specs, check_vma=False)
```

```python
import functools

import jax
import jax.numpy as jnp
from jax import lax
from jax.experimental import pallas as pl
from jax.experimental.pallas import tpu as pltpu
from jax.sharding import PartitionSpec as P


F32 = jnp.float32
BF16 = jnp.bfloat16
HIGH = lax.Precision.HIGHEST
NS_ITERS = 5
CHIPS = 8
SHARE = 4
VARS = 4
LINES = 128
WIDTH = 512
HALF = 32
CAP = 32
OBS = 512
BLOCK = SHARE * VARS * 4 * 8
MB = 1 << 20


ALL_VMEM = 67_043_328


def params(mib=None):
    return pltpu.CompilerParams(vmem_limit_bytes=ALL_VMEM if mib is None else mib * MB)


def vmem():
    return pl.BlockSpec(memory_space=pltpu.VMEM)


def base_row(chunk, chip):
    if chunk == 0:
        return 32 + 8 * chip
    return 8 * chip + jnp.where(chip >= 4, 64, 0)


def stencil_tiles(chunk, win, m, here, before, behind, base, low, high, spread, mix, out):
    row = lax.broadcasted_iota(jnp.int32, (8, WIDTH), 0)
    lane = lax.broadcasted_iota(jnp.int32, (8, WIDTH), 1)
    tiles = [win[m, v, pl.ds(here, 8), :] for v in range(VARS)]
    for v in range(VARS):
        t = tiles[v]
        prev = pltpu.roll(win[m, v, pl.ds(before, 8), :], 1, 0)
        nxt = pltpu.roll(win[m, v, pl.ds(behind, 8), :], 7, 0)
        if chunk == 1:
            prev = jnp.where(base == 0, pltpu.roll(low[m, v], 1, 0), prev)
            nxt = jnp.where(base == LINES - 8, pltpu.roll(high[m, v], 7, 0), nxt)
        up = jnp.where(row == 0, prev, pltpu.roll(t, 1, 0))
        down = jnp.where(row == 7, nxt, pltpu.roll(t, 7, 0))
        left = jnp.where(lane == 0, 0.0, pltpu.roll(t, 1, 1))
        right = jnp.where(lane == WIDTH - 1, 0.0, pltpu.roll(t, WIDTH - 1, 1))
        laplace = down + up + right + left - 4.0 * t
        mixing = mix[v, 0] * tiles[0]
        for w in range(1, VARS):
            mixing = mixing + mix[v, w] * tiles[w]
        res = t + spread[v] * laplace + mixing
        for q in range(4):
            at = m * 128 + (v * 4 + q) * 8
            if not isinstance(m, int):
                at = pl.multiple_of(at, 8)
            out[pl.ds(at, 8), :] = res[:, q * 128 : (q + 1) * 128]


def first_kernel(spread_in, mix_in, x, out, win, buf, spread, mix, in_sems, out_sems, scalar_sems):
    chip = lax.axis_index("mem") // 2
    start = pl.multiple_of(base_row(0, lax.rem(chip + FIRST, CHIPS)) - 8, 8)
    copies = [
        pltpu.make_async_copy(x.at[m, :, pl.ds(start, 24), :], win.at[m], in_sems.at[m]) for m in range(SHARE)
    ]
    scalars = [
        pltpu.make_async_copy(spread_in, spread, scalar_sems.at[0]),
        pltpu.make_async_copy(mix_in, mix, scalar_sems.at[1]),
    ]
    for copy in scalars + copies:
        copy.start()
    for copy in scalars:
        copy.wait()
    done = []
    for m in range(SHARE):
        copies[m].wait()
        stencil_tiles(0, win, m, 8, 0, 16, None, None, None, spread, mix, buf)
        rows = pl.ds(m * 128, 128)
        copy = pltpu.make_async_copy(buf.at[rows, :], out.at[rows, :], out_sems.at[m])
        copy.start()
        done.append(copy)
    for copy in done:
        copy.wait()


def first_stencil(spread, mix, x):
    return pl.pallas_call(
        first_kernel,
        in_specs=[hbm()] * 3,
        out_specs=hbm(),
        out_shape=jax.ShapeDtypeStruct((BLOCK, 128), F32),
        scratch_shapes=[
            pltpu.VMEM((SHARE, VARS, 24, WIDTH), F32),
            pltpu.VMEM((BLOCK, 128), F32),
            pltpu.SMEM((VARS,), F32),
            pltpu.SMEM((VARS, VARS), F32),
            pltpu.SemaphoreType.DMA((SHARE,)),
            pltpu.SemaphoreType.DMA((SHARE,)),
            pltpu.SemaphoreType.DMA((2,)),
        ],
        compiler_params=params(),
        cost_estimate=pl.CostEstimate(flops=2_500_000, bytes_accessed=MB, transcendentals=0),
        name="stencil_a1",
    )(spread, mix, x)


def stencil_kernel(chunk, dists, part, *refs):
    low = high = obs_in = placed = None
    if part == "next":
        *obs_in, spread_in, mix_in, x = refs[:9]
        refs = refs[9:]
    elif part == "b":
        low, high, spread_in, mix_in, x = refs[:5]
        refs = refs[5:]
    else:
        placed, spread_in, mix_in, x = refs[:4]
        refs = refs[4:]
    outs, refs = refs[: len(dists)], refs[len(dists) :]
    if part == "next":
        placed, far, *refs = refs
    if part == "rest":
        first_out, last_out, *refs = refs
    win, spread, mix, sems, scalar_sems = refs
    chip = lax.axis_index("mem") // 2
    bases, starts, copies = [], [], []
    for k, d in enumerate(dists):
        base = pl.multiple_of(base_row(chunk, lax.rem(chip + d, CHIPS)), 8)
        start = base - 8 if chunk == 0 else jnp.clip(base - 8, 0, LINES - 24)
        start = pl.multiple_of(start, 8)
        copy = pltpu.make_async_copy(x.at[:, :, pl.ds(start, 24), :], win.at[k], sems.at[k])
        copy.start()
        bases.append(base)
        starts.append(start)
        copies.append(copy)
    scalars = [
        pltpu.make_async_copy(spread_in, spread, scalar_sems.at[0]),
        pltpu.make_async_copy(mix_in, mix, scalar_sems.at[1]),
    ]
    for copy in scalars:
        copy.start()
    edges = []
    if part == "rest":
        edges = [
            pltpu.make_async_copy(x.at[:, :, pl.ds(0, 8), :], first_out, sems.at[len(dists)]),
            pltpu.make_async_copy(x.at[:, :, pl.ds(LINES - 8, 8), :], last_out, sems.at[len(dists) + 1]),
        ]
        for copy in edges:
            copy.start()
    if part == "next":
        placed[...] = place_obs(*obs_in)
    if chunk == 0:
        targets = [(d, outs[k].at[BLOCK : BLOCK + 8]) for k, d in enumerate(dists)]
        if part == "next":
            targets.append((FIRST, far))
        for d, ref in targets:
            lanes = pl.multiple_of(lax.rem(chip + d, CHIPS) * 128, 128)
            ref[...] = placed[:, pl.ds(lanes, 128)]
    for copy in scalars:
        copy.wait()
    for k in range(len(dists)):
        base = bases[k]
        copies[k].wait()
        if chunk == 0:
            here, before, behind = 8, 0, 16
        else:
            here = pl.multiple_of(base - starts[k], 8)
            before = pl.multiple_of(jnp.maximum(here - 8, 0), 8)
            behind = pl.multiple_of(jnp.minimum(here + 8, 16), 8)

        def member(m, _, k=k, base=base, here=here, before=before, behind=behind):
            stencil_tiles(chunk, win.at[k], m, here, before, behind, base, low, high, spread, mix, outs[k])
            return 0

        lax.fori_loop(0, SHARE, member, 0)
    for copy in edges:
        copy.wait()


def hbm():
    return pl.BlockSpec(memory_space=pltpu.HBM)


def stencil(chunk, dists, part, extra, spread, mix, x):
    n = len(dists)
    rows = BLOCK + 8 if chunk == 0 else BLOCK
    more = []
    if part == "next":
        more = [jax.ShapeDtypeStruct((8, 2 * OBS), F32), jax.ShapeDtypeStruct((8, 128), F32)]
    if part == "rest":
        more = [jax.ShapeDtypeStruct((SHARE, VARS, 8, WIDTH), F32)] * 2
    res = pl.pallas_call(
        functools.partial(stencil_kernel, chunk, dists, part),
        in_specs=[vmem()] * len(extra) + [hbm()] * 3,
        out_specs=[vmem()] * (n + len(more)),
        out_shape=[jax.ShapeDtypeStruct((rows, 128), F32)] * n + more,
        scratch_shapes=[
            pltpu.VMEM((n, SHARE, VARS, 24, WIDTH), F32),
            pltpu.SMEM((VARS,), F32),
            pltpu.SMEM((VARS, VARS), F32),
            pltpu.SemaphoreType.DMA((n + 2,)),
            pltpu.SemaphoreType.DMA((2,)),
        ],
        compiler_params=params(),
        cost_estimate=pl.CostEstimate(flops=2_500_000 * n, bytes_accessed=n * MB, transcendentals=0),
    )(*extra, spread, mix, x)
    return dict(zip(dists, res[:n])), res[n:]


def parts3(x):
    a = x.astype(BF16)
    r = x - a.astype(F32)
    b = r.astype(BF16)
    c = (r - b.astype(F32)).astype(BF16)
    return a, b, c


def nt(a, b):
    return lax.dot_general(a, b, (((1,), (1,)), ((), ())), preferred_element_type=F32)


def place_obs(pid, tidx, entry, value, inv, table):
    ids = pid[...]
    sub = lax.broadcasted_iota(jnp.int32, (32, OBS), 0)
    named = sub == jnp.broadcast_to(ids, (32, OBS))
    onehot = jnp.where(named, 1.0, 0.0)
    earlier = jnp.where(
        lax.broadcasted_iota(jnp.int32, (OBS, OBS), 0) < lax.broadcasted_iota(jnp.int32, (OBS, OBS), 1),
        1.0, 0.0,
    ).astype(BF16)
    before = jnp.dot(onehot.astype(BF16), earlier, preferred_element_type=F32)
    rank = jnp.sum(before * onehot, axis=0, keepdims=True).astype(jnp.int32)
    inner = (ids >= 8) & (ids < 24)
    group = jnp.where(inner, 2 * (ids - 8), jnp.where(ids < 8, 2 * ids + 1, 2 * (ids - 16) + 1))
    target = group * CAP + rank
    levels = table.shape[1]
    look = jnp.where(
        lax.broadcasted_iota(jnp.int32, (levels, OBS), 0) == jnp.broadcast_to(tidx[...], (levels, OBS)),
        1.0, 0.0,
    ).astype(BF16)
    taper = sum(
        jnp.dot(jnp.broadcast_to(p, (16, levels)), look, preferred_element_type=F32)
        for p in parts3(table[...])
    )
    weight = inv[...] * taper[0:1]
    c = entry[...]
    place = (c & 0x1800) | ((c & 0x180) << 2) | ((c & 0x600) >> 2) | (c & 0x7F)
    r8 = lax.broadcasted_iota(jnp.int32, (16, OBS), 0)
    fields = jnp.where(
        r8 == 0, jnp.broadcast_to(value[...], (16, OBS)),
        jnp.where(r8 == 1, jnp.broadcast_to(weight, (16, OBS)),
                  jnp.where(r8 == 2, jnp.broadcast_to(place.astype(F32), (16, OBS)), 0.0)),
    )
    pieces = parts3(fields)
    halves = []
    for k in range(2):
        slots = jnp.where(
            lax.broadcasted_iota(jnp.int32, (OBS, OBS), 0) + k * OBS == jnp.broadcast_to(target, (OBS, OBS)),
            1.0, 0.0,
        ).astype(BF16)
        placed = nt(pieces[0], slots) + nt(pieces[1], slots) + nt(pieces[2], slots)
        halves.append(placed[0:8])
    return jnp.concatenate(halves, axis=1)


def gather_members_kernel(chunk, *refs):
    blocks, refs = refs[:CHIPS], refs[CHIPS:]
    if chunk == 0:
        far, *refs = refs
    keep, send = refs
    core = lax.axis_index("mem") % 2
    own = 4 * core
    for g in range(64):
        vl, r = g // 4, g % 4
        for d in range(CHIPS):
            keep[g, pl.ds(SHARE * d, SHARE), :] = blocks[d][pl.ds(vl * 8 + r + own, SHARE, stride=128), :]
            send[g, pl.ds(SHARE * d, SHARE), :] = blocks[d][pl.ds(vl * 8 + r + 4 - own, SHARE, stride=128), :]
    if chunk == 0:
        quarter = lax.broadcasted_iota(jnp.int32, (8, 128), 1) // CAP
        for out, whose in ((keep, core), (send, 1 - core)):
            for q in range(4):
                first = whose * 64 + (q // 2) * CAP
                packed = jnp.zeros((8, 128), F32)
                for k in range(4):
                    d = (q % 2) * 4 + k
                    tile = far[...] if d == FIRST else blocks[d][BLOCK : BLOCK + 8, :]
                    moved = pltpu.roll(tile, (k * CAP - first) & 127, 1)
                    packed = jnp.where(quarter == k, moved, packed)
                out[64, pl.ds(q * 8, 8), :] = packed


def gather_members(chunk, blocks):
    half = jax.ShapeDtypeStruct((65 if chunk == 0 else 64, HALF, 128), F32)
    return pl.pallas_call(
        functools.partial(gather_members_kernel, chunk),
        in_specs=[vmem()] * len(blocks),
        out_specs=[vmem()] * 2,
        out_shape=[half] * 2,
        compiler_params=params(16),
        cost_estimate=pl.CostEstimate(flops=20_000_000, bytes_accessed=4 * MB, transcendentals=0),
    )(*blocks)


def spread_members_kernel(keep, came, *outs):
    own = 4 * (lax.axis_index("mem") % 2)
    for d in range(CHIPS):
        for m in range(SHARE):
            for vl in range(16):
                at = (m * 16 + vl) * 8
                start = vl * 128 + d * SHARE + m
                outs[d][pl.ds(at + own, 4), :] = keep[pl.ds(start, 4, stride=HALF), :]
                outs[d][pl.ds(at + 4 - own, 4), :] = came[pl.ds(start, 4, stride=HALF), :]


def spread_members(keep, came):
    return pl.pallas_call(
        spread_members_kernel,
        in_specs=[vmem()] * 2,
        out_specs=[vmem()] * CHIPS,
        out_shape=[jax.ShapeDtypeStruct((BLOCK, 128), F32)] * CHIPS,
        compiler_params=params(16),
        cost_estimate=pl.CostEstimate(flops=20_000_000, bytes_accessed=4 * MB, transcendentals=0),
    )(keep.reshape(64 * HALF, 128), came.reshape(64 * HALF, 128))


def high(a, b):
    return jnp.dot(a, b, precision=HIGH, preferred_element_type=F32)


def analysis_kernel(chunk, keep, came, *refs):
    if chunk == 0:
        out_keep, out_send, later, parts, centres, acc = refs
        tiles = [[half[64, q * 8 : (q + 1) * 8, :] for half in (keep, came) for q in pair] for pair in ((0, 1), (2, 3))]
        obs = jnp.concatenate(tiles[0], axis=1)
        later[...] = jnp.concatenate(tiles[1], axis=1)
    else:
        obs_in, out_keep, out_send, parts, centres, acc = refs
        obs = obs_in[...]
    members = 2 * HALF
    acc[...] = jnp.zeros_like(acc)
    cell = lax.broadcasted_iota(jnp.int32, (256, OBS), 0)
    where_obs = obs[2:3, :].astype(jnp.int32)

    def select(t, _):
        g = 2 * t
        cols = [jnp.concatenate([keep[g + h], came[g + h]], axis=0) for h in range(2)]
        block = jnp.concatenate(cols, axis=1)
        centre = jnp.sum(block, axis=0, keepdims=True) * (1.0 / members)
        dev = block - centre
        hi = dev.astype(BF16)
        lo = (dev - hi.astype(F32)).astype(BF16)
        c1 = centre.astype(BF16)
        rest = centre - c1.astype(F32)
        c2 = rest.astype(BF16)
        c3 = rest - c2.astype(F32)
        row = lax.broadcasted_iota(jnp.int32, (16, 256), 0)
        crows = jnp.where(
            row == 0, jnp.broadcast_to(c1.astype(F32), (16, 256)),
            jnp.where(row == 1, jnp.broadcast_to(c2.astype(F32), (16, 256)),
                      jnp.where(row == 2, jnp.broadcast_to(c3, (16, 256)), 0.0)),
        ).astype(BF16)
        both = jnp.concatenate([hi, lo], axis=0)
        parts[t] = both
        centres[t] = jnp.broadcast_to(centre, (8, 256))
        chosen = jnp.where(cell == jnp.broadcast_to(where_obs - t * 256, (256, OBS)), 1.0, 0.0).astype(BF16)
        acc[...] += jnp.dot(jnp.concatenate([both, crows], axis=0), chosen, preferred_element_type=F32)
        return 0

    lax.fori_loop(0, 32, select, 0)
    columns = acc[0:members] + acc[members : 2 * members]
    centre_obs = acc[128:129] + acc[129:130] + acc[130:131]
    innovation = obs[0:1, :] - centre_obs
    weight = obs[1:2, :]
    weighted = columns * weight
    pair = (((1,), (1,)), ((), ()))
    gram = lax.dot_general(weighted, columns, pair, precision=HIGH, preferred_element_type=F32)
    drive = lax.dot_general(
        jnp.broadcast_to(weight * innovation, (8, OBS)), columns, pair, precision=HIGH, preferred_element_type=F32
    )
    eye = jnp.where(
        lax.broadcasted_iota(jnp.int32, (members, members), 0) == lax.broadcasted_iota(jnp.int32, (members, members), 1),
        1.0, 0.0,
    )
    system = (members - 1.0) * eye + gram
    norm = jnp.sqrt(jnp.sum(jnp.sum(system * system, axis=1, keepdims=True), axis=0, keepdims=True))
    y = system / norm
    z = 1.5 * eye - 0.5 * y
    y = high(y, z)
    for sweep in range(1, NS_ITERS):
        mid = 1.5 * eye - 0.5 * high(z, y)
        if sweep < NS_ITERS - 1:
            y = high(y, mid)
        z = high(mid, z)
    root = z / jnp.sqrt(norm)
    offset = high(high(drive, root), root)
    coeff = offset[0:1, :] + jnp.sqrt(members - 1.0) * root
    spread = jnp.where(
        lax.broadcasted_iota(jnp.int32, (members, 256), 0)
        == (lax.broadcasted_iota(jnp.int32, (members, 256), 1) & (members - 1)),
        1.0, 0.0,
    )
    four = high(coeff, spread)
    four_hi = four.astype(BF16)
    four_lo = four - four_hi.astype(F32)
    lanes = lax.broadcasted_iota(jnp.int32, (members, 256), 1)
    left = jnp.where(lanes < 128, four_hi.astype(F32), four_lo).astype(BF16)

    def transform(t, _):
        g = 2 * t
        both = parts[t]
        res = jnp.dot(left, jnp.concatenate([both, both], axis=0), preferred_element_type=F32)
        res = res + jnp.broadcast_to(centres[t][0:1], (members, 256))
        for h in range(2):
            out_keep[g + h] = res[0:HALF, h * 128 : (h + 1) * 128]
            out_send[g + h] = res[HALF:members, h * 128 : (h + 1) * 128]
        return 0

    lax.fori_loop(0, 32, transform, 0)


def analysis(chunk, keep, came, obs):
    half = jax.ShapeDtypeStruct((64, HALF, 128), F32)
    later = [jax.ShapeDtypeStruct((8, OBS), F32)] if chunk == 0 else []
    return pl.pallas_call(
        functools.partial(analysis_kernel, chunk),
        in_specs=[vmem()] * (2 + len(obs)),
        out_specs=[vmem()] * (2 + len(later)),
        out_shape=[half] * 2 + later,
        scratch_shapes=[
            pltpu.VMEM((32, 128, 256), BF16),
            pltpu.VMEM((32, 8, 256), F32),
            pltpu.VMEM((144, OBS), F32),
        ],
        compiler_params=params(24),
        cost_estimate=pl.CostEstimate(flops=100_000_000, bytes_accessed=4 * MB, transcendentals=0),
    )(keep, came, *obs)


def assemble_kernel(chunk, dists, *refs):
    *refs, out, tiles, sems = refs
    blocks = refs[-len(dists) :]
    chip = lax.axis_index("mem") // 2
    copies = []
    for k, d in enumerate(dists):
        for m in range(SHARE):
            for v in range(VARS):
                for q in range(4):
                    at = (m * 16 + v * 4 + q) * 8
                    tiles[k, m, v, :, q * 128 : (q + 1) * 128] = blocks[k][at : at + 8, :]
        base = pl.multiple_of(base_row(chunk, lax.rem(chip + d, CHIPS)), 8)
        copy = pltpu.make_async_copy(tiles.at[k], out.at[:, :, pl.ds(base, 8), :], sems.at[k])
        copy.start()
        copies.append(copy)
    for copy in copies:
        copy.wait()


def assemble(chunk, dists, grid, blocks):
    n = len(dists)
    kept = [] if grid is None else [grid]
    return pl.pallas_call(
        functools.partial(assemble_kernel, chunk, dists),
        in_specs=[hbm()] * len(kept) + [vmem()] * n,
        out_specs=hbm(),
        out_shape=jax.ShapeDtypeStruct((SHARE, VARS, LINES, WIDTH), F32),
        scratch_shapes=[pltpu.VMEM((n, SHARE, VARS, 8, WIDTH), F32), pltpu.SemaphoreType.DMA((n,))],
        input_output_aliases={0: 0} if kept else {},
        compiler_params=params(8),
        cost_estimate=pl.CostEstimate(flops=1_000_000 * n, bytes_accessed=n * MB // 2, transcendentals=0),
    )(*kept, *[blocks[d] for d in dists])


def hop(block, d):
    n = 2 * CHIPS
    return lax.ppermute(block, "mem", [(i, (i + 2 * d) % n) for i in range(n)])


ORDER = (4, 3, 5, 2, 6, 1, 7)
ALL = ORDER + (0,)
FIRST = ORDER[0]
PIECES = ((4, 0, 5), (3, 6, 2), (1, 7))


def exchange(blocks, dists, sign):
    got = {}
    for d in dists:
        if d == 0:
            got[d] = blocks[d]
            continue
        got[d] = hop(blocks[d], sign * d)
    return got


def swap(x):
    return lax.ppermute(x, "mem", [(i, i ^ 1) for i in range(2 * CHIPS)])


def shards(
    prior_ensemble,
    spreading_factor,
    tendency_matrix,
    measured_data,
    inverse_error,
    assigned_subregion,
    measured_entry,
    taper_index,
    taper_factors,
):
    x = prior_ensemble
    physics = (spreading_factor, tendency_matrix, x)

    obs = (
        assigned_subregion.reshape(1, OBS), taper_index, measured_entry, measured_data,
        inverse_error, taper_factors.reshape(1, -1),
    )
    sent = {FIRST: first_stencil(*physics)}
    got_a = exchange(sent, ALL[:1], 1)
    sent, (placed, far) = stencil(0, ALL[1:3], "next", obs, *physics)
    got_a |= exchange(sent, ALL[1:3], 1)
    sent, (first, last) = stencil(0, ALL[3:], "rest", (placed,), *physics)
    got_a |= exchange(sent, ALL[3:], 1)
    far = hop(far, FIRST)

    count = lax.axis_size("dom")
    forward = [(i, i + 1) for i in range(count - 1)]
    backward = [(b, a) for a, b in forward]
    low = lax.ppermute(last, "dom", forward)
    high_row = lax.ppermute(first, "dom", backward)
    sent_b, _ = stencil(1, ALL, "b", (low, high_row), *physics)
    got_b = exchange(sent_b, ALL, 1)

    back, slots = [], []
    for chunk, got in enumerate((got_a, got_b)):
        blocks = [got[d] for d in range(CHIPS)] + ([far] if chunk == 0 else [])
        keep, send = gather_members(chunk, blocks)
        came = swap(send)
        out_keep, out_send, *slots = analysis(chunk, keep, came, slots)
        returned = swap(out_send)
        outs = spread_members(out_keep, returned)
        back.append(exchange(dict(enumerate(outs)), ALL, -1))
    grid = assemble(0, ALL, None, back[0])
    for dists in PIECES:
        grid = assemble(1, dists, grid, back[1])
    return grid


def solution(mesh):
    in_specs = (
        P("mem", None, "dom", None),
        P(),
        P(),
        P("dom", "mem"),
        P("dom", "mem"),
        P("dom", "mem", None),
        P("dom", "mem"),
        P("dom", "mem"),
        P(),
    )
    out_specs = P("mem", None, "dom", None)

    return jax.shard_map(shards, mesh=mesh, in_specs=in_specs, out_specs=out_specs, check_vma=False)
```

```python
import functools

import jax
import jax.numpy as jnp
from jax import lax
from jax.experimental import pallas as pl
from jax.experimental.pallas import tpu as pltpu
from jax.sharding import PartitionSpec as P


F32 = jnp.float32
BF16 = jnp.bfloat16
HIGH = lax.Precision.HIGHEST
NS_ITERS = 5
CHIPS = 8
SHARE = 4
VARS = 4
LINES = 128
WIDTH = 512
HALF = 32
CAP = 32
OBS = 512
BLOCK = SHARE * VARS * 4 * 8
MB = 1 << 20


ALL_VMEM = 67_043_328


def params(mib=None):
    return pltpu.CompilerParams(vmem_limit_bytes=ALL_VMEM if mib is None else mib * MB)


def vmem():
    return pl.BlockSpec(memory_space=pltpu.VMEM)


def base_row(chunk, chip):
    if chunk == 0:
        return 32 + 8 * chip
    return 8 * chip + jnp.where(chip >= 4, 64, 0)


def stencil_tiles(chunk, win, m, here, before, behind, base, low, high, spread, mix, out):
    row = lax.broadcasted_iota(jnp.int32, (8, WIDTH), 0)
    lane = lax.broadcasted_iota(jnp.int32, (8, WIDTH), 1)
    tiles = [win[m, v, pl.ds(here, 8), :] for v in range(VARS)]
    for v in range(VARS):
        t = tiles[v]
        prev = pltpu.roll(win[m, v, pl.ds(before, 8), :], 1, 0)
        nxt = pltpu.roll(win[m, v, pl.ds(behind, 8), :], 7, 0)
        if chunk == 1:
            prev = jnp.where(base == 0, pltpu.roll(low[m, v], 1, 0), prev)
            nxt = jnp.where(base == LINES - 8, pltpu.roll(high[m, v], 7, 0), nxt)
        up = jnp.where(row == 0, prev, pltpu.roll(t, 1, 0))
        down = jnp.where(row == 7, nxt, pltpu.roll(t, 7, 0))
        left = jnp.where(lane == 0, 0.0, pltpu.roll(t, 1, 1))
        right = jnp.where(lane == WIDTH - 1, 0.0, pltpu.roll(t, WIDTH - 1, 1))
        laplace = down + up + right + left - 4.0 * t
        mixing = mix[v, 0] * tiles[0]
        for w in range(1, VARS):
            mixing = mixing + mix[v, w] * tiles[w]
        res = t + spread[v] * laplace + mixing
        for q in range(4):
            at = m * 128 + (v * 4 + q) * 8
            if not isinstance(m, int):
                at = pl.multiple_of(at, 8)
            out[pl.ds(at, 8), :] = res[:, q * 128 : (q + 1) * 128]


def first_kernel(spread_in, mix_in, x, out, win, spread, mix, in_sems, scalar_sems):
    chip = lax.axis_index("mem") // 2
    start = pl.multiple_of(base_row(0, lax.rem(chip + FIRST, CHIPS)) - 8, 8)
    copies = [
        pltpu.make_async_copy(x.at[m, :, pl.ds(start, 24), :], win.at[m], in_sems.at[m]) for m in range(SHARE)
    ]
    scalars = [
        pltpu.make_async_copy(spread_in, spread, scalar_sems.at[0]),
        pltpu.make_async_copy(mix_in, mix, scalar_sems.at[1]),
    ]
    for copy in scalars + copies:
        copy.start()
    for copy in scalars:
        copy.wait()
    for m in range(SHARE):
        copies[m].wait()
        stencil_tiles(0, win, m, 8, 0, 16, None, None, None, spread, mix, out)


def first_stencil(spread, mix, x):
    return pl.pallas_call(
        first_kernel,
        in_specs=[hbm()] * 3,
        out_specs=vmem(),
        out_shape=jax.ShapeDtypeStruct((BLOCK, 128), F32),
        scratch_shapes=[
            pltpu.VMEM((SHARE, VARS, 24, WIDTH), F32),
            pltpu.SMEM((VARS,), F32),
            pltpu.SMEM((VARS, VARS), F32),
            pltpu.SemaphoreType.DMA((SHARE,)),
            pltpu.SemaphoreType.DMA((2,)),
        ],
        compiler_params=params(8),
        cost_estimate=pl.CostEstimate(flops=2_500_000, bytes_accessed=MB, transcendentals=0),
        name="stencil_a1",
    )(spread, mix, x)


def stencil_kernel(chunk, dists, part, *refs):
    low = high = obs_in = placed = None
    if part == "next":
        *obs_in, spread_in, mix_in, x = refs[:9]
        refs = refs[9:]
    elif part == "b":
        low, high, spread_in, mix_in, x = refs[:5]
        refs = refs[5:]
    else:
        placed, spread_in, mix_in, x = refs[:4]
        refs = refs[4:]
    outs, refs = refs[: len(dists)], refs[len(dists) :]
    if part == "next":
        placed, far, *refs = refs
    if part == "rest":
        first_out, last_out, *refs = refs
    win, spread, mix, sems, scalar_sems = refs
    chip = lax.axis_index("mem") // 2
    bases, starts, copies = [], [], []
    for k, d in enumerate(dists):
        base = pl.multiple_of(base_row(chunk, lax.rem(chip + d, CHIPS)), 8)
        start = base - 8 if chunk == 0 else jnp.clip(base - 8, 0, LINES - 24)
        start = pl.multiple_of(start, 8)
        copy = pltpu.make_async_copy(x.at[:, :, pl.ds(start, 24), :], win.at[k], sems.at[k])
        copy.start()
        bases.append(base)
        starts.append(start)
        copies.append(copy)
    scalars = [
        pltpu.make_async_copy(spread_in, spread, scalar_sems.at[0]),
        pltpu.make_async_copy(mix_in, mix, scalar_sems.at[1]),
    ]
    for copy in scalars:
        copy.start()
    edges = []
    if part == "rest":
        edges = [
            pltpu.make_async_copy(x.at[:, :, pl.ds(0, 8), :], first_out, sems.at[len(dists)]),
            pltpu.make_async_copy(x.at[:, :, pl.ds(LINES - 8, 8), :], last_out, sems.at[len(dists) + 1]),
        ]
        for copy in edges:
            copy.start()
    if part == "next":
        placed[...] = place_obs(*obs_in)
    if chunk == 0:
        targets = [(d, outs[k].at[BLOCK : BLOCK + 8]) for k, d in enumerate(dists)]
        if part == "next":
            targets.append((FIRST, far))
        for d, ref in targets:
            lanes = pl.multiple_of(lax.rem(chip + d, CHIPS) * 128, 128)
            ref[...] = placed[:, pl.ds(lanes, 128)]
    for copy in scalars:
        copy.wait()
    for k in range(len(dists)):
        base = bases[k]
        copies[k].wait()
        if chunk == 0:
            here, before, behind = 8, 0, 16
        else:
            here = pl.multiple_of(base - starts[k], 8)
            before = pl.multiple_of(jnp.maximum(here - 8, 0), 8)
            behind = pl.multiple_of(jnp.minimum(here + 8, 16), 8)

        def member(m, _, k=k, base=base, here=here, before=before, behind=behind):
            stencil_tiles(chunk, win.at[k], m, here, before, behind, base, low, high, spread, mix, outs[k])
            return 0

        lax.fori_loop(0, SHARE, member, 0)
    for copy in edges:
        copy.wait()


def hbm():
    return pl.BlockSpec(memory_space=pltpu.HBM)


def stencil(chunk, dists, part, extra, spread, mix, x):
    n = len(dists)
    rows = BLOCK + 8 if chunk == 0 else BLOCK
    more = []
    if part == "next":
        more = [jax.ShapeDtypeStruct((8, 2 * OBS), F32), jax.ShapeDtypeStruct((8, 128), F32)]
    if part == "rest":
        more = [jax.ShapeDtypeStruct((SHARE, VARS, 8, WIDTH), F32)] * 2
    res = pl.pallas_call(
        functools.partial(stencil_kernel, chunk, dists, part),
        in_specs=[vmem()] * len(extra) + [hbm()] * 3,
        out_specs=[vmem()] * (n + len(more)),
        out_shape=[jax.ShapeDtypeStruct((rows, 128), F32)] * n + more,
        scratch_shapes=[
            pltpu.VMEM((n, SHARE, VARS, 24, WIDTH), F32),
            pltpu.SMEM((VARS,), F32),
            pltpu.SMEM((VARS, VARS), F32),
            pltpu.SemaphoreType.DMA((n + 2,)),
            pltpu.SemaphoreType.DMA((2,)),
        ],
        compiler_params=params(24),
        cost_estimate=pl.CostEstimate(flops=2_500_000 * n, bytes_accessed=n * MB, transcendentals=0),
    )(*extra, spread, mix, x)
    return dict(zip(dists, res[:n])), res[n:]


def parts3(x):
    a = x.astype(BF16)
    r = x - a.astype(F32)
    b = r.astype(BF16)
    c = (r - b.astype(F32)).astype(BF16)
    return a, b, c


def nt(a, b):
    return lax.dot_general(a, b, (((1,), (1,)), ((), ())), preferred_element_type=F32)


def place_obs(pid, tidx, entry, value, inv, table):
    ids = pid[...]
    sub = lax.broadcasted_iota(jnp.int32, (32, OBS), 0)
    named = sub == jnp.broadcast_to(ids, (32, OBS))
    onehot = jnp.where(named, 1.0, 0.0)
    earlier = jnp.where(
        lax.broadcasted_iota(jnp.int32, (OBS, OBS), 0) < lax.broadcasted_iota(jnp.int32, (OBS, OBS), 1),
        1.0, 0.0,
    ).astype(BF16)
    before = jnp.dot(onehot.astype(BF16), earlier, preferred_element_type=F32)
    rank = jnp.sum(before * onehot, axis=0, keepdims=True).astype(jnp.int32)
    inner = (ids >= 8) & (ids < 24)
    group = jnp.where(inner, 2 * (ids - 8), jnp.where(ids < 8, 2 * ids + 1, 2 * (ids - 16) + 1))
    target = group * CAP + rank
    levels = table.shape[1]
    look = jnp.where(
        lax.broadcasted_iota(jnp.int32, (levels, OBS), 0) == jnp.broadcast_to(tidx[...], (levels, OBS)),
        1.0, 0.0,
    ).astype(BF16)
    taper = sum(
        jnp.dot(jnp.broadcast_to(p, (16, levels)), look, preferred_element_type=F32)
        for p in parts3(table[...])
    )
    weight = inv[...] * taper[0:1]
    c = entry[...]
    place = (c & 0x1800) | ((c & 0x180) << 2) | ((c & 0x600) >> 2) | (c & 0x7F)
    r8 = lax.broadcasted_iota(jnp.int32, (16, OBS), 0)
    fields = jnp.where(
        r8 == 0, jnp.broadcast_to(value[...], (16, OBS)),
        jnp.where(r8 == 1, jnp.broadcast_to(weight, (16, OBS)),
                  jnp.where(r8 == 2, jnp.broadcast_to(place.astype(F32), (16, OBS)), 0.0)),
    )
    pieces = parts3(fields)
    halves = []
    for k in range(2):
        slots = jnp.where(
            lax.broadcasted_iota(jnp.int32, (OBS, OBS), 0) + k * OBS == jnp.broadcast_to(target, (OBS, OBS)),
            1.0, 0.0,
        ).astype(BF16)
        placed = nt(pieces[0], slots) + nt(pieces[1], slots) + nt(pieces[2], slots)
        halves.append(placed[0:8])
    return jnp.concatenate(halves, axis=1)


def gather_members_kernel(chunk, *refs):
    blocks, refs = refs[:CHIPS], refs[CHIPS:]
    if chunk == 0:
        far, *refs = refs
    keep, send = refs
    core = lax.axis_index("mem") % 2
    own = 4 * core
    for g in range(64):
        vl, r = g // 4, g % 4
        for d in range(CHIPS):
            keep[g, pl.ds(SHARE * d, SHARE), :] = blocks[d][pl.ds(vl * 8 + r + own, SHARE, stride=128), :]
            send[g, pl.ds(SHARE * d, SHARE), :] = blocks[d][pl.ds(vl * 8 + r + 4 - own, SHARE, stride=128), :]
    if chunk == 0:
        quarter = lax.broadcasted_iota(jnp.int32, (8, 128), 1) // CAP
        for out, whose in ((keep, core), (send, 1 - core)):
            for q in range(4):
                first = whose * 64 + (q // 2) * CAP
                packed = jnp.zeros((8, 128), F32)
                for k in range(4):
                    d = (q % 2) * 4 + k
                    tile = far[...] if d == FIRST else blocks[d][BLOCK : BLOCK + 8, :]
                    moved = pltpu.roll(tile, (k * CAP - first) & 127, 1)
                    packed = jnp.where(quarter == k, moved, packed)
                out[64, pl.ds(q * 8, 8), :] = packed


def gather_members(chunk, blocks):
    half = jax.ShapeDtypeStruct((65 if chunk == 0 else 64, HALF, 128), F32)
    return pl.pallas_call(
        functools.partial(gather_members_kernel, chunk),
        in_specs=[vmem()] * len(blocks),
        out_specs=[vmem()] * 2,
        out_shape=[half] * 2,
        compiler_params=params(16),
        cost_estimate=pl.CostEstimate(flops=20_000_000, bytes_accessed=4 * MB, transcendentals=0),
    )(*blocks)


def spread_members_kernel(keep, came, *outs):
    own = 4 * (lax.axis_index("mem") % 2)
    for d in range(CHIPS):
        for m in range(SHARE):
            for vl in range(16):
                at = (m * 16 + vl) * 8
                start = vl * 128 + d * SHARE + m
                outs[d][pl.ds(at + own, 4), :] = keep[pl.ds(start, 4, stride=HALF), :]
                outs[d][pl.ds(at + 4 - own, 4), :] = came[pl.ds(start, 4, stride=HALF), :]


def spread_members(keep, came):
    return pl.pallas_call(
        spread_members_kernel,
        in_specs=[vmem()] * 2,
        out_specs=[vmem()] * CHIPS,
        out_shape=[jax.ShapeDtypeStruct((BLOCK, 128), F32)] * CHIPS,
        compiler_params=params(16),
        cost_estimate=pl.CostEstimate(flops=20_000_000, bytes_accessed=4 * MB, transcendentals=0),
    )(keep.reshape(64 * HALF, 128), came.reshape(64 * HALF, 128))


def high(a, b):
    return jnp.dot(a, b, precision=HIGH, preferred_element_type=F32)


def analysis_kernel(chunk, keep, came, *refs):
    if chunk == 0:
        out_keep, out_send, later, parts, centres, acc = refs
        tiles = [[half[64, q * 8 : (q + 1) * 8, :] for half in (keep, came) for q in pair] for pair in ((0, 1), (2, 3))]
        obs = jnp.concatenate(tiles[0], axis=1)
        later[...] = jnp.concatenate(tiles[1], axis=1)
    else:
        obs_in, out_keep, out_send, parts, centres, acc = refs
        obs = obs_in[...]
    members = 2 * HALF
    acc[...] = jnp.zeros_like(acc)
    cell = lax.broadcasted_iota(jnp.int32, (256, OBS), 0)
    where_obs = obs[2:3, :].astype(jnp.int32)

    def select(t, _):
        g = 2 * t
        cols = [jnp.concatenate([keep[g + h], came[g + h]], axis=0) for h in range(2)]
        block = jnp.concatenate(cols, axis=1)
        centre = jnp.sum(block, axis=0, keepdims=True) * (1.0 / members)
        dev = block - centre
        hi = dev.astype(BF16)
        lo = (dev - hi.astype(F32)).astype(BF16)
        c1 = centre.astype(BF16)
        rest = centre - c1.astype(F32)
        c2 = rest.astype(BF16)
        c3 = rest - c2.astype(F32)
        row = lax.broadcasted_iota(jnp.int32, (16, 256), 0)
        crows = jnp.where(
            row == 0, jnp.broadcast_to(c1.astype(F32), (16, 256)),
            jnp.where(row == 1, jnp.broadcast_to(c2.astype(F32), (16, 256)),
                      jnp.where(row == 2, jnp.broadcast_to(c3, (16, 256)), 0.0)),
        ).astype(BF16)
        both = jnp.concatenate([hi, lo], axis=0)
        parts[t] = both
        centres[t] = jnp.broadcast_to(centre, (8, 256))
        chosen = jnp.where(cell == jnp.broadcast_to(where_obs - t * 256, (256, OBS)), 1.0, 0.0).astype(BF16)
        acc[...] += jnp.dot(jnp.concatenate([both, crows], axis=0), chosen, preferred_element_type=F32)
        return 0

    lax.fori_loop(0, 32, select, 0)
    columns = acc[0:members] + acc[members : 2 * members]
    centre_obs = acc[128:129] + acc[129:130] + acc[130:131]
    innovation = obs[0:1, :] - centre_obs
    weight = obs[1:2, :]
    weighted = columns * weight
    pair = (((1,), (1,)), ((), ()))
    gram = lax.dot_general(weighted, columns, pair, precision=HIGH, preferred_element_type=F32)
    drive = lax.dot_general(
        jnp.broadcast_to(weight * innovation, (8, OBS)), columns, pair, precision=HIGH, preferred_element_type=F32
    )
    eye = jnp.where(
        lax.broadcasted_iota(jnp.int32, (members, members), 0) == lax.broadcasted_iota(jnp.int32, (members, members), 1),
        1.0, 0.0,
    )
    system = (members - 1.0) * eye + gram
    norm = jnp.sqrt(jnp.sum(jnp.sum(system * system, axis=1, keepdims=True), axis=0, keepdims=True))
    y = system / norm
    z = 1.5 * eye - 0.5 * y
    y = high(y, z)
    for sweep in range(1, NS_ITERS):
        mid = 1.5 * eye - 0.5 * high(z, y)
        if sweep < NS_ITERS - 1:
            y = high(y, mid)
        z = high(mid, z)
    root = z / jnp.sqrt(norm)
    offset = high(high(drive, root), root)
    coeff = offset[0:1, :] + jnp.sqrt(members - 1.0) * root
    spread = jnp.where(
        lax.broadcasted_iota(jnp.int32, (members, 256), 0)
        == (lax.broadcasted_iota(jnp.int32, (members, 256), 1) & (members - 1)),
        1.0, 0.0,
    )
    four = high(coeff, spread)
    four_hi = four.astype(BF16)
    four_lo = four - four_hi.astype(F32)
    lanes = lax.broadcasted_iota(jnp.int32, (members, 256), 1)
    left = jnp.where(lanes < 128, four_hi.astype(F32), four_lo).astype(BF16)

    def transform(t, _):
        g = 2 * t
        both = parts[t]
        res = jnp.dot(left, jnp.concatenate([both, both], axis=0), preferred_element_type=F32)
        res = res + jnp.broadcast_to(centres[t][0:1], (members, 256))
        for h in range(2):
            out_keep[g + h] = res[0:HALF, h * 128 : (h + 1) * 128]
            out_send[g + h] = res[HALF:members, h * 128 : (h + 1) * 128]
        return 0

    lax.fori_loop(0, 32, transform, 0)


def analysis(chunk, keep, came, obs):
    half = jax.ShapeDtypeStruct((64, HALF, 128), F32)
    later = [jax.ShapeDtypeStruct((8, OBS), F32)] if chunk == 0 else []
    return pl.pallas_call(
        functools.partial(analysis_kernel, chunk),
        in_specs=[vmem()] * (2 + len(obs)),
        out_specs=[vmem()] * (2 + len(later)),
        out_shape=[half] * 2 + later,
        scratch_shapes=[
            pltpu.VMEM((32, 128, 256), BF16),
            pltpu.VMEM((32, 8, 256), F32),
            pltpu.VMEM((144, OBS), F32),
        ],
        compiler_params=params(24),
        cost_estimate=pl.CostEstimate(flops=100_000_000, bytes_accessed=4 * MB, transcendentals=0),
    )(keep, came, *obs)


def assemble_kernel(chunk, dists, *refs):
    *refs, out, tiles, sems = refs
    blocks = refs[-len(dists) :]
    chip = lax.axis_index("mem") // 2
    copies = []
    for k, d in enumerate(dists):
        for m in range(SHARE):
            for v in range(VARS):
                for q in range(4):
                    at = (m * 16 + v * 4 + q) * 8
                    tiles[k, m, v, :, q * 128 : (q + 1) * 128] = blocks[k][at : at + 8, :]
        base = pl.multiple_of(base_row(chunk, lax.rem(chip + d, CHIPS)), 8)
        copy = pltpu.make_async_copy(tiles.at[k], out.at[:, :, pl.ds(base, 8), :], sems.at[k])
        copy.start()
        copies.append(copy)
    for copy in copies:
        copy.wait()


def assemble(chunk, dists, grid, blocks):
    n = len(dists)
    kept = [] if grid is None else [grid]
    return pl.pallas_call(
        functools.partial(assemble_kernel, chunk, dists),
        in_specs=[hbm()] * len(kept) + [vmem()] * n,
        out_specs=hbm(),
        out_shape=jax.ShapeDtypeStruct((SHARE, VARS, LINES, WIDTH), F32),
        scratch_shapes=[pltpu.VMEM((n, SHARE, VARS, 8, WIDTH), F32), pltpu.SemaphoreType.DMA((n,))],
        input_output_aliases={0: 0} if kept else {},
        compiler_params=params(8),
        cost_estimate=pl.CostEstimate(flops=1_000_000 * n, bytes_accessed=n * MB // 2, transcendentals=0),
    )(*kept, *[blocks[d] for d in dists])


def hop(block, d):
    n = 2 * CHIPS
    return lax.ppermute(block, "mem", [(i, (i + 2 * d) % n) for i in range(n)])


ORDER = (4, 3, 5, 2, 6, 1, 7)
ALL = ORDER + (0,)
FIRST = ORDER[0]
PIECES = ((4, 0, 5), (3, 6, 2), (1, 7))


def exchange(blocks, dists, sign):
    got = {}
    for d in dists:
        if d == 0:
            got[d] = blocks[d]
            continue
        got[d] = hop(blocks[d], sign * d)
    return got


def swap(x):
    return lax.ppermute(x, "mem", [(i, i ^ 1) for i in range(2 * CHIPS)])


def shards(
    prior_ensemble,
    spreading_factor,
    tendency_matrix,
    measured_data,
    inverse_error,
    assigned_subregion,
    measured_entry,
    taper_index,
    taper_factors,
):
    x, spreading_factor, tendency_matrix = [
        pltpu.with_memory_space_constraint(a, pltpu.HBM) for a in (prior_ensemble, spreading_factor, tendency_matrix)
    ]
    physics = (spreading_factor, tendency_matrix, x)

    obs = (
        assigned_subregion.reshape(1, OBS), taper_index, measured_entry, measured_data,
        inverse_error, taper_factors.reshape(1, -1),
    )
    sent = {FIRST: first_stencil(*physics)}
    got_a = exchange(sent, ALL[:1], 1)
    sent, (placed, far) = stencil(0, ALL[1:3], "next", obs, *physics)
    got_a |= exchange(sent, ALL[1:3], 1)
    sent, (first, last) = stencil(0, ALL[3:], "rest", (placed,), *physics)
    got_a |= exchange(sent, ALL[3:], 1)
    far = hop(far, FIRST)

    count = lax.axis_size("dom")
    forward = [(i, i + 1) for i in range(count - 1)]
    backward = [(b, a) for a, b in forward]
    low = lax.ppermute(last, "dom", forward)
    high_row = lax.ppermute(first, "dom", backward)
    sent_b, _ = stencil(1, ALL, "b", (low, high_row), *physics)
    got_b = exchange(sent_b, ALL, 1)

    back, slots = [], []
    for chunk, got in enumerate((got_a, got_b)):
        blocks = [got[d] for d in range(CHIPS)] + ([far] if chunk == 0 else [])
        keep, send = gather_members(chunk, blocks)
        came = swap(send)
        out_keep, out_send, *slots = analysis(chunk, keep, came, slots)
        returned = swap(out_send)
        outs = spread_members(out_keep, returned)
        back.append(exchange(dict(enumerate(outs)), ALL, -1))
    grid = assemble(0, ALL, None, back[0])
    for dists in PIECES:
        grid = assemble(1, dists, grid, back[1])
    return grid


def solution(mesh):
    in_specs = (
        P("mem", None, "dom", None),
        P(),
        P(),
        P("dom", "mem"),
        P("dom", "mem"),
        P("dom", "mem", None),
        P("dom", "mem"),
        P("dom", "mem"),
        P(),
    )
    out_specs = P("mem", None, "dom", None)

    return jax.shard_map(shards, mesh=mesh, in_specs=in_specs, out_specs=out_specs, check_vma=False)
```
